32 devices in a mesh: dp: 2 (over x), tp: 16 (over y, z, core).
Axes of the slice: x: 2, y: 2, z: 4, core: 2. Of those that a mesh axis runs over, the one named last changes fastest.
Arguments:
- x: bfloat16 [8, 512, 8192], P('dp'), parts along dimension 0
- gain_a: bfloat16 [8192], replicated
- wq: bfloat16 [8192, 8192], P(None, 'tp')
- wk: bfloat16 [8192, 8192], P(None, 'tp')
- wv: bfloat16 [8192, 8192], P(None, 'tp')
- wo: bfloat16 [8192, 8192], P('tp')
- gain_m: bfloat16 [8192], replicated
- w_gate: bfloat16 [8192, 24576], P(None, 'tp')
- w_up: bfloat16 [8192, 24576], P(None, 'tp')
- w_down: bfloat16 [24576, 8192], P('tp')
Outputs:
- output: bfloat16 [8, 512, 8192], P('dp'), parts along dimension 0
There are 2 independent parts. The reference program is written for one: setup_inputs(seed, part) draws one part's arguments, and reference() takes and returns one part's arrays. A program takes and returns all parts, laid end to end along the dimension named above; an argument that names none is the same for every part.
All inputs are finite; a program needn't handle non-finite values.
Results may differ from the reference program's by a relative error of at most 0.017.
Values are sent between devices in bfloat16 or wider.
A program may use at most 2 GiB of HBM per device.

```python
import jax
import jax.numpy as jnp
from jax import lax

SEQUENCES = 4
TOKENS = 512
D = 8192
HEADS = 64
KV_HEADS = 64
HEAD = 128
FF = 24576
THETA = 10000


def setup_inputs(seed: int = 0, part: int = 0) -> dict:
    kx, ka, km, kq, kk, kv, ko, kg, ku, kd = jax.random.split(jax.random.key(seed), 10)

    def weights(key, rows, columns):
        return jax.random.normal(key, (rows, columns), jnp.float32) * rows**-0.5

    drawn = {
        "x": jax.random.normal(jax.random.fold_in(kx, part), (SEQUENCES, TOKENS, D), jnp.float32),
        "gain_a": 1 + 0.1 * jax.random.normal(ka, (D,), jnp.float32),
        "wq": 2 * weights(kq, D, HEADS * HEAD),
        "wk": 2 * weights(kk, D, KV_HEADS * HEAD),
        "wv": 4 * weights(kv, D, KV_HEADS * HEAD),
        "wo": weights(ko, HEADS * HEAD, D),
        "gain_m": 1 + 0.1 * jax.random.normal(km, (D,), jnp.float32),
        "w_gate": weights(kg, D, FF),
        "w_up": weights(ku, D, FF),
        "w_down": 3 * weights(kd, FF, D),
    }
    return {k: v.astype(jnp.bfloat16) for k, v in drawn.items()}


def normed(x, gain):
    wide = x.astype(jnp.float32)
    scale = lax.rsqrt(jnp.mean(wide * wide, -1, keepdims=True) + 1e-6)
    return (wide * scale * gain.astype(jnp.float32)).astype(jnp.bfloat16)


def turned(t, place, theta):
    half = t.shape[-1] // 2
    angle = place.astype(jnp.float32)[:, None] * theta ** (-jnp.arange(half, dtype=jnp.float32) / half)
    cos, sin = jnp.cos(angle)[:, None], jnp.sin(angle)[:, None]
    a, b = t[..., :half].astype(jnp.float32), t[..., half:].astype(jnp.float32)
    return jnp.concatenate([a * cos - b * sin, b * cos + a * sin], -1).astype(jnp.bfloat16)


def matmul(a, w):
    return jnp.dot(a, w, preferred_element_type=jnp.float32).astype(jnp.bfloat16)


def einsum(form, a, b):
    return jnp.einsum(form, a.astype(jnp.float32), b.astype(jnp.float32))


def attention(q, k, v):
    scores = einsum("tgsd,ugd->gstu", q, k) * q.shape[-1] ** -0.5
    token = jnp.arange(q.shape[0])
    scores = jnp.where(token[:, None] >= token, scores, -jnp.inf)
    weights = jax.nn.softmax(scores, -1).astype(jnp.bfloat16)
    return einsum("gstu,ugd->tgsd", weights, v).astype(jnp.bfloat16)


def one(x, gain_a, wq, wk, wv, wo, gain_m, w_gate, w_up, w_down):
    rows = x.shape[0]
    a, place = normed(x, gain_a), jnp.arange(rows)
    k = turned(matmul(a, wk).reshape(rows, -1, HEAD), place, THETA)
    q = turned(matmul(a, wq).reshape(rows, -1, HEAD), place, THETA).reshape(rows, k.shape[1], -1, HEAD)
    v = matmul(a, wv).reshape(rows, -1, HEAD)
    seen = attention(q, k, v).reshape(rows, -1)
    h = (x.astype(jnp.float32) + jnp.dot(seen, wo, preferred_element_type=jnp.float32)).astype(jnp.bfloat16)
    b = normed(h, gain_m)
    gate = jnp.dot(b, w_gate, preferred_element_type=jnp.float32)
    up = jnp.dot(b, w_up, preferred_element_type=jnp.float32)
    hidden = (jax.nn.silu(gate) * up).astype(jnp.bfloat16)
    return (h.astype(jnp.float32) + jnp.dot(hidden, w_down, preferred_element_type=jnp.float32)).astype(jnp.bfloat16)


def reference(x, gain_a, wq, wk, wv, wo, gain_m, w_gate, w_up, w_down):
    return lax.map(lambda sequence: one(sequence, gain_a, wq, wk, wv, wo, gain_m, w_gate, w_up, w_down), x)
```

```python
import functools

import jax
import jax.numpy as jnp
from jax import lax
from jax.experimental import pallas as pl
from jax.experimental.pallas import tpu as pltpu
from jax.sharding import PartitionSpec as P

HEAD = 128
THETA = 10000
F32, BF16 = jnp.float32, jnp.bfloat16

R = 256
RH = R // 2
C = RH // 8
NI = 8
NT = 2 * NI
D, HW, FL = 8192, 512, 1536
CY = 4864
CZ = D - CY
KH, GK, PW = D // 2, 1024, 512
NS = 8
AT = {"sd": (0, 0), "s0": (0, 1), "s1": (0, 6), "s2": (1, 3), "s3": (2, 0), "s4": (2, 5), "s5": (3, 2), "s6": (3, 7), "s7": (4, 4), "s8": (5, 1), "s9": (5, 3)}
LAST = NT - 1 + 5

SEMS = ["D", "YR", "ZR", "gZR", "gYR", "gD"] + [f"{g}{p}{s}{j}" for g in ("", "g") for p in "YZ" for s in "+-" for j in (1, 2, 3)]
SEM = {n: i for i, n in enumerate(SEMS)}


def _dot(a, b, ca=1, cb=0):
    return lax.dot_general(a, b, (((ca,), (cb,)), ((), ())), preferred_element_type=F32)


def kernel(x_ref, ga_ref, gm_ref, cos_ref, sin_ref, wq_ref, wk_ref, wv_ref, wo_ref, wg_ref, wu_ref, wd_ref, yb_ref,
           own, oth, drx, yrs, yrr, yls, ylr, zls, zlr, zrs, zrr, och, xch, hst, ablk, wsl, acc, hid, kst, vst, seen,
           ssem, rsem, cred, wsem, asem, xsem, osem):
    t = lax.axis_index("tp")
    c, z, y = lax.rem(t, 2), lax.rem(lax.div(t, 2), 4), lax.div(t, 8)

    def at(y_, z_, c_):
        return (y_ * 4 + z_) * 2 + c_

    peer = {"c": at(y, z, 1 - c), "y": at(1 - y, z, c), "+": at(y, jnp.minimum(z + 1, 3), c), "-": at(y, jnp.maximum(z - 1, 0), c)}

    def signal(sem, to):
        pl.semaphore_signal(sem, inc=1, device_id={"tp": peer[to]}, device_id_type=pl.DeviceIdType.MESH)

    def each_peer(fn):
        fn("c")
        fn("y")
        pl.when(z > 0)(lambda: fn("-"))
        pl.when(z < 3)(lambda: fn("+"))

    barrier = pltpu.get_barrier_semaphore()
    each_peer(lambda p: signal(barrier, p))
    pl.when((z == 0) | (z == 3))(lambda: pl.semaphore_wait(barrier, 3))
    pl.when((z > 0) & (z < 3))(lambda: pl.semaphore_wait(barrier, 4))

    def rdma(name, par, src, dst, to):
        return pltpu.make_async_remote_copy(src_ref=src, dst_ref=dst, send_sem=ssem.at[SEM[name]], recv_sem=rsem.at[SEM[name], par],
                                            device_id={"tp": peer[to]}, device_id_type=pl.DeviceIdType.MESH)

    NW = NI * 8 + NI * 24

    def fetch(w):
        slot = lax.rem(w, 3)
        sem = wsem.at[slot]

        def go(src, lo, n):
            pltpu.make_async_copy(src, wsl.at[slot, pl.ds(lo, n), :], sem).start()

        @pl.when(w < NI * 8)
        def _():
            j = lax.rem(w, 8)
            h = lax.rem(j, 2)
            for n, ref in enumerate((wq_ref, wk_ref, wv_ref)):
                pl.when(lax.div(j, 2) == n)(lambda ref=ref: go(ref.at[pl.ds(h * KH, KH), :], 0, KH))

            @pl.when(j >= 6)
            def _():
                for p in range(8):
                    go(wo_ref.at[:, pl.ds(h * KH + p * PW, PW)], p * HW, HW)

        @pl.when((w >= NI * 8) & (w < NW))
        def _():
            u = lax.rem(w - NI * 8, 24)
            for n, ref in enumerate((wg_ref, wu_ref)):
                @pl.when((u < 16) & (lax.rem(u, 2) == n))
                def _(ref=ref):
                    for p in range(3):
                        go(ref.at[pl.ds(lax.div(u, 2) * GK, GK), pl.ds(p * PW, PW)], p * GK, GK)

            @pl.when(u >= 16)
            def _():
                for p in range(2):
                    go(wd_ref.at[:, pl.ds((u - 16) * 2 * PW + p * PW, PW)], p * FL, FL)

    def tile_wait(w, rows):
        slot = lax.rem(w, 3)
        ref = wsl.at[slot, pl.ds(0, rows), :]
        pltpu.make_async_copy(ref, ref, wsem.at[slot]).wait()
        fetch(w + 2)
        return slot

    def rows_start(job):
        slot = lax.rem(job, 2)

        @pl.when(job < NI)
        def _():
            for q in range(16):
                pltpu.make_async_copy(x_ref.at[job, q // 8, (q // 4) % 2, q % 4], ablk.at[slot, pl.ds(q * C, C), :], asem.at[slot]).start()

        @pl.when((job >= NI) & (job < NT))
        def _():
            for q in range(16):
                half = lax.rem(c + q // 8, 2)
                pltpu.make_async_copy(yb_ref.at[job - NI, half, (q // 4) % 2, q % 4], ablk.at[slot, pl.ds(q * C, C), :], asem.at[slot]).start()

    def rows_wait(job):
        slot = lax.rem(job, 2)
        pltpu.make_async_copy(ablk.at[slot], ablk.at[slot], asem.at[slot]).wait()
        return slot

    def put(job, out, col):
        cols = pl.ds(pl.multiple_of(col, PW), PW)
        own[lax.rem(job, 4), :, :, :, cols] = out[:RH].reshape(2, 4, C, PW)
        oth[:, :, :, cols] = out[RH:].astype(BF16).reshape(2, 4, C, PW)

    def attention_slice(job, n):
        w = job * 8 + n
        ab = lax.rem(job, 2)
        half = lax.rem(job, 2)

        @pl.when(n == 0)
        def _():
            rows_wait(job)

            def norm(g, _):
                rows = pl.ds(pl.multiple_of(g * 16, 16), 16)
                v = ablk[ab, rows, :].astype(F32)
                scale = lax.rsqrt(jnp.mean(v * v, -1, keepdims=True) + 1e-6)
                ablk[ab, rows, :] = (v * scale * ga_ref[...].astype(F32)).astype(BF16)

            lax.fori_loop(0, R // 16, norm, None)
            acc[0] = jnp.zeros((R, FL), F32)

        slot = tile_wait(w, KH)

        @pl.when(n < 6)
        def _():
            cols = pl.ds(pl.multiple_of(lax.div(n, 2) * PW, PW), PW)

            def part(k, _):
                lhs = ablk[ab, :, pl.ds(pl.multiple_of(lax.rem(n, 2) * KH + k * GK, GK), GK)]
                acc[0, :, cols] += _dot(lhs, wsl[slot, pl.ds(pl.multiple_of(k * GK, GK), GK), :])

            lax.fori_loop(0, KH // GK, part, None)

        @pl.when(n == 5)
        def _():
            place = pl.ds(pl.multiple_of(half * R, R), R)

            def head(i, _):
                cos, sin = cos_ref[place, :], sin_ref[place, :]

                def column(first):
                    return acc[0, :, pl.ds(pl.multiple_of(first + i * HEAD, HEAD), HEAD)].astype(BF16)

                def turn(first):
                    v = column(first).astype(F32)
                    return (v * cos + pltpu.roll(v, HEAD // 2, 1) * sin).astype(BF16)

                q = turn(0)
                kst[i, place, :] = turn(PW)
                vst[i, place, :] = column(2 * PW)

                def attend(seen_keys):
                    s = _dot(q, kst[i, :seen_keys, :], 1, 1) * HEAD**-0.5
                    token = lax.broadcasted_iota(jnp.int32, s.shape, 0) + (seen_keys - R)
                    s = jnp.where(token >= lax.broadcasted_iota(jnp.int32, s.shape, 1), s, -1e30)
                    p = jnp.exp(s - s.max(-1, keepdims=True))
                    p = (p * (1 / p.sum(-1, keepdims=True))).astype(BF16)
                    o = _dot(p, vst[i, :seen_keys, :]).astype(BF16)
                    cols = pl.ds(pl.multiple_of(i * HEAD, HEAD), HEAD)
                    seen[pl.ds(pl.multiple_of(c * RH, RH), RH), cols] = o[:RH]
                    seen[pl.ds(pl.multiple_of((1 - c) * RH, RH), RH), cols] = o[RH:]

                pl.when(half == 0)(lambda: attend(R))
                pl.when(half == 1)(lambda: attend(2 * R))

            lax.fori_loop(0, HW // HEAD, head, None)

        @pl.when(n >= 6)
        def _():
            def part(p, _):
                put(job, _dot(seen[...], wsl[slot, pl.ds(pl.multiple_of(p * HW, HW), HW), :]), (n - 6) * KH + p * PW)

            lax.fori_loop(0, 8, part, None)

    def mlp_slice(job, n):
        ab = lax.rem(job, 2)

        @pl.when(n == 0)
        def _():
            rows_wait(job)
            acc[...] = jnp.zeros((2, R, FL), F32)

        def one(q, _):
            u = n * 3 + q
            w = NI * 8 + (job - NI) * 24 + u
            slot = tile_wait(w, 3 * GK)

            @pl.when(u < 16)
            def _():
                lhs = ablk[ab, :, pl.ds(pl.multiple_of(lax.div(u, 2) * GK, GK), GK)]
                which = lax.rem(u, 2)
                for p in range(3):
                    acc[which, :, p * PW : (p + 1) * PW] += _dot(lhs, wsl[slot, p * GK : (p + 1) * GK, :])

            @pl.when(u == 15)
            def _():
                def rows(g, _):
                    r = pl.ds(pl.multiple_of(g * 16, 16), 16)
                    gate = acc[0, r, :]
                    hid[r, :] = (gate * (1 / (1 + jnp.exp(-gate))) * acc[1, r, :]).astype(BF16)

                lax.fori_loop(0, R // 16, rows, None)

            @pl.when(u >= 16)
            def _():
                for p in range(2):
                    put(job, _dot(hid[...], wsl[slot, p * FL : (p + 1) * FL, :]), (u - 16) * 2 * PW + p * PW)

        lax.fori_loop(0, 3, one, None)

    def rs_send(s, j):
        return ((z < 3) & (j > z), 4 + z - j) if s == "+" else ((z > 0) & (j >= 4 - z), j + z - 4)

    def rs_recv(s, j):
        return (z >= 1) & (j >= z) if s == "+" else (z <= 2) & (j >= 3 - z)

    def first(s):
        return z == 0 if s == "+" else z == 3

    def ag_send(s, j):
        return ((z < 3) & (j <= z + 1), z - (j - 1)) if s == "+" else ((z > 0) & (j <= 4 - z), z + (j - 1))

    def ag_recv(s, j):
        return ((z >= 1) & (j <= z), z - j) if s == "+" else ((z <= 2) & (j <= 3 - z), z + j)

    YC, ZC = pl.ds(0, CY), pl.ds(CY, CZ)
    S = {"+": 0, "-": 1}

    def sd(i, par):
        rdma("D", 0, oth, drx, "c").start()

    def y_line(i, par, j):
        for s in "+-":
            yes, k = rs_send(s, j)

            @pl.when(yes & first(s))
            def _():
                yls[S[s], j - 1] = own[lax.rem(i, 4), y, k, :, YC].astype(BF16)

            if j > 1:
                @pl.when(yes & ~first(s))
                def _():
                    yls[S[s], j - 1] = (own[lax.rem(i, 4), y, k, :, YC] + ylr[par, S[s], j - 2].astype(F32)).astype(BF16)

            pl.when(yes)(rdma(f"Y{s}{j}", par, yls.at[S[s], j - 1], ylr.at[par, S[s], j - 1], s).start)

    def z_line(i, par, j):
        for s in "+-":
            yes, k = rs_send(s, j)

            @pl.when(yes & first(s))
            def _():
                for h in range(2):
                    zls[S[s], j - 1, h] = own[lax.rem(i, 4), h, k, :, ZC].astype(BF16)

            if j > 1:
                @pl.when(yes & ~first(s))
                def _():
                    for h in range(2):
                        zls[S[s], j - 1, h] = (own[lax.rem(i, 4), h, k, :, ZC] + zlr[par, S[s], j - 2, h].astype(F32)).astype(BF16)

            pl.when(yes)(rdma(f"Z{s}{j}", par, zls.at[S[s], j - 1], zlr.at[par, S[s], j - 1], s).start)

    def line_wait(part, par, j):
        sb, rb = (yls, ylr) if part == "Y" else (zls, zlr)
        for s in "+-":
            cp = rdma(f"{part}{s}{j}", par, sb.at[S[s], j - 1], rb.at[par, S[s], j - 1], s)
            pl.when(rs_send(s, j)[0])(cp.wait_send)
            pl.when(rs_recv(s, j))(cp.wait_recv)

    def s0(i, par):
        rdma("D", 0, oth, drx, "c").wait()
        slot = lax.rem(i, 4)

        def add(k, _):
            a, b = lax.div(k, 4), lax.rem(k, 4)
            own[slot, a, b] += drx[a, b].astype(F32)

        lax.fori_loop(0, 8, add, None)

        def cast(k, _):
            yrs[k] = own[slot, 1 - y, k, :, YC].astype(BF16)

        lax.fori_loop(0, 4, cast, None)
        rdma("YR", par, yrs, yrr.at[par], "y").start()
        z_line(i, par, 1)

    def s1(i, par):
        rdma("YR", par, yrs, yrr.at[par], "y").wait()
        slot = lax.rem(i, 4)

        def add(k, _):
            own[slot, y, k, :, YC] += yrr[par, k].astype(F32)

        lax.fori_loop(0, 4, add, None)
        y_line(i, par, 1)
        line_wait("Z", par, 1)
        z_line(i, par, 2)

    def s2(i, par):
        line_wait("Y", par, 1)
        y_line(i, par, 2)
        line_wait("Z", par, 2)
        z_line(i, par, 3)

    def x_copy(i):
        return pltpu.make_async_copy(x_ref.at[i, c, y, z], xch, xsem)

    def s3(i, par):
        pl.when(i < NI)(lambda: x_copy(i).start())
        line_wait("Y", par, 2)
        y_line(i, par, 3)
        line_wait("Z", par, 3)
        slot = lax.rem(i, 4)
        for s in "+-":
            @pl.when(rs_recv(s, 3))
            def _():
                for h in range(2):
                    own[slot, h, z, :, ZC] += zlr[par, S[s], 2, h].astype(F32)
        zrs[...] = own[slot, 1 - y, z, :, ZC].astype(BF16)
        rdma("ZR", par, zrs, zrr.at[par], "y").start()

    def och_copy(i):
        return pltpu.make_async_copy(och, yb_ref.at[i, c, y, z], osem)

    def ag_first(i, par):
        cps = [(ag_send(s, 1)[0], ag_recv(s, 1)[0], rdma(f"gY{s}1", par, och.at[:, YC], yb_ref.at[i, c, y, z, :, YC], s)) for s in "+-"]
        return cps, rdma("gZR", par, och.at[:, ZC], yb_ref.at[i, c, y, z, :, ZC], "y")

    def s4(i, par):
        slot = lax.rem(i, 4)
        line_wait("Y", par, 3)
        for s in "+-":
            @pl.when(rs_recv(s, 3))
            def _():
                own[slot, y, z, :, YC] += ylr[par, S[s], 2].astype(F32)
        rdma("ZR", par, zrs, zrr.at[par], "y").wait()
        own[slot, y, z, :, ZC] += zrr[par].astype(F32)

        @pl.when(i < NI)
        def _():
            x_copy(i).wait()
            h = (xch[...].astype(F32) + own[slot, y, z]).astype(BF16)
            hst[i] = h
            v = h.astype(F32)
            scale = lax.rsqrt(jnp.mean(v * v, -1, keepdims=True) + 1e-6)
            och[...] = (v * scale * gm_ref[...].astype(F32)).astype(BF16)

        @pl.when(i >= NI)
        def _():
            och[...] = (hst[i - NI].astype(F32) + own[slot, y, z]).astype(BF16)

        och_copy(i).start()
        lines, rung = ag_first(i, par)
        for yes, _, cp in lines:
            pl.when(yes)(cp.start)
        rung.start()

    def ag_y(i, par, j):
        return [(*ag_send(s, j), *ag_recv(s, j), s) for s in "+-"]

    def g_src(part, i, k):
        return yb_ref.at[i, c, y, k, :, YC] if part == "Y" else yb_ref.at[i, c, :, k, :, ZC]

    def g_line(part, i, par, j):
        for s in "+-":
            yes, k = ag_send(s, j)

            @pl.when(yes)
            def _():
                rdma(f"g{part}{s}{j}", par, g_src(part, i, k), g_src(part, i, k), s).start()

    def g_wait(part, i, par, j):
        for s in "+-":
            yes, k = ag_send(s, j)
            got, _ = ag_recv(s, j)
            ref = g_src(part, i, 0)
            cp = rdma(f"g{part}{s}{j}", par, ref, ref, s)
            pl.when(yes)(cp.wait_send)
            pl.when(got)(cp.wait_recv)

    def s5(i, par):
        och_copy(i).wait()
        lines, rung = ag_first(i, par)
        for yes, got, cp in lines:
            pl.when(yes)(cp.wait_send)
            pl.when(got)(cp.wait_recv)
        g_line("Y", i, par, 2)
        rung.wait()
        g_line("Z", i, par, 1)

    def s6(i, par):
        g_wait("Y", i, par, 2)
        g_line("Y", i, par, 3)
        g_wait("Z", i, par, 1)
        g_line("Z", i, par, 2)

    def g_rung(i, par):
        ref = yb_ref.at[i, c, y, :, :, YC]
        return rdma("gYR", par, ref, ref, "y")

    def g_core(i, par):
        ref = yb_ref.at[i, c]
        return rdma("gD", par, ref, ref, "c")

    def s7(i, par):
        g_wait("Y", i, par, 3)
        g_rung(i, par).start()
        g_wait("Z", i, par, 2)
        g_line("Z", i, par, 3)

    def s8(i, par):
        g_rung(i, par).wait()
        g_wait("Z", i, par, 3)
        g_core(i, par).start()

    def s9(i, par):
        g_core(i, par).wait()

    actions = [("sd", sd), ("s0", s0), ("s1", s1), ("s2", s2), ("s3", s3), ("s4", s4), ("s5", s5), ("s6", s6), ("s7", s7), ("s8", s8), ("s9", s9)]
    order = sorted(actions, key=lambda a: -AT[a[0]][0])

    CR = {"c": 0, "y": 1, "-": 2, "+": 3}
    BACK = {"c": 0, "y": 1, "-": 3, "+": 2}

    rows_start(0)
    fetch(0)
    fetch(1)

    def body(m, _):
        k, n = lax.div(m, NS) - 1, lax.rem(m, NS)
        pl.when((n == 0) & (k >= 1))(lambda: each_peer(lambda p: pl.semaphore_wait(cred.at[CR[p]], 1)))
        for name, fn in order:
            d, pos = AT[name]
            i = k - d
            pl.when((n == pos) & (i >= 0) & (i < NT))(lambda fn=fn, i=i: fn(i, lax.rem(i, 2)))
        job = k + 1
        pl.when(n == 4)(lambda: rows_start(k + 2))
        pl.when(job < NI)(lambda: attention_slice(job, n))
        pl.when((job >= NI) & (job < NT))(lambda: mlp_slice(job, n))
        pl.when((n == NS - 1) & (k >= 0) & (k < LAST))(lambda: each_peer(lambda p: signal(cred.at[BACK[p]], p)))

    lax.fori_loop(0, (LAST + 2) * NS, body, None)


def solution(mesh):
    def step(x, gain_a, wq, wk, wv, wo, gain_m, w_gate, w_up, w_down):
        batch, rows, d = x.shape
        place = jnp.arange(rows, dtype=F32)[:, None]
        half = HEAD // 2
        angle = place * THETA ** (-jnp.arange(half, dtype=F32) / half)
        cos, sin = jnp.cos(angle), jnp.sin(angle)
        cos, sin = jnp.concatenate([cos, cos], -1), jnp.concatenate([-sin, sin], -1)
        hbm, vmem = pl.BlockSpec(memory_space=pl.ANY), pl.BlockSpec(memory_space=pltpu.VMEM)
        yb = pl.pallas_call(
            kernel,
            out_shape=jax.ShapeDtypeStruct((NT, 2, 2, 4, C, D), BF16),
            in_specs=[hbm, vmem, vmem, vmem, vmem] + [hbm] * 7,
            out_specs=hbm,
            scratch_shapes=[
                pltpu.VMEM((4, 2, 4, C, D), F32),
                pltpu.VMEM((2, 4, C, D), BF16),
                pltpu.VMEM((2, 4, C, D), BF16),
                pltpu.VMEM((4, C, CY), BF16),
                pltpu.VMEM((2, 4, C, CY), BF16),
                pltpu.VMEM((2, 3, C, CY), BF16),
                pltpu.VMEM((2, 2, 3, C, CY), BF16),
                pltpu.VMEM((2, 3, 2, C, CZ), BF16),
                pltpu.VMEM((2, 2, 3, 2, C, CZ), BF16),
                pltpu.VMEM((C, CZ), BF16),
                pltpu.VMEM((2, C, CZ), BF16),
                pltpu.VMEM((C, D), BF16),
                pltpu.VMEM((C, D), BF16),
                pltpu.VMEM((NI, C, D), BF16),
                pltpu.VMEM((2, R, D), BF16),
                pltpu.VMEM((3, KH, PW), BF16),
                pltpu.VMEM((2, R, FL), F32),
                pltpu.VMEM((R, FL), BF16),
                pltpu.VMEM((HW // HEAD, 2 * R, HEAD), BF16),
                pltpu.VMEM((HW // HEAD, 2 * R, HEAD), BF16),
                pltpu.VMEM((R, HW), BF16),
                pltpu.SemaphoreType.DMA((len(SEMS),)),
                pltpu.SemaphoreType.DMA((len(SEMS), 2)),
                pltpu.SemaphoreType.REGULAR((4,)),
                pltpu.SemaphoreType.DMA((3,)),
                pltpu.SemaphoreType.DMA((2,)),
                pltpu.SemaphoreType.DMA,
                pltpu.SemaphoreType.DMA,
            ],
            compiler_params=pltpu.CompilerParams(collective_id=0, has_side_effects=True, vmem_limit_bytes=67043328),
            name="layer",
        )(x.reshape(NI, 2, 2, 4, C, D), gain_a.reshape(1, d), gain_m.reshape(1, d), cos, sin, wq, wk, wv, wo, w_gate, w_up, w_down)
        return yb[NI:].reshape(x.shape)

    tokens, whole, columns, rows_of = P("dp", None, None), P(None), P(None, "tp"), P("tp", None)
    return jax.shard_map(
        step,
        mesh=mesh,
        in_specs=(tokens, whole, columns, columns, columns, rows_of, whole, columns, columns, rows_of),
        out_specs=tokens,
        check_vma=False,
    )
```

```python
import functools
import math

import jax
import jax.numpy as jnp
from jax import lax
from jax.experimental import pallas as pl
from jax.experimental.pallas import tpu as pltpu
from jax.sharding import PartitionSpec as P

HEAD = 128
THETA = 10000
F32, BF16 = jnp.float32, jnp.bfloat16

JR = 256
R = JR // 2
RH = R // 2
C = RH // 8
NJ = 8
NI = 2 * NJ
NT = 2 * NI
OS = 7
OT = 4
D, HW, FL = 8192, 512, 1536
CY = 4864
CZ = D - CY
KH, GK, PW = D // 2, 1024, 512
NS = 8
AT = {"sd": (0, 0), "s0": (0, 1), "s1": (0, 6), "s2": (1, 3), "s3": (2, 0), "s4": (2, 5), "s5": (3, 2), "s6": (3, 7), "s7": (4, 4), "s8": (5, 2), "s9": (5, 4)}
LAST = NT - 1 + 5

SEMS = ["D", "YR", "ZR", "gZR", "gYR", "gD"] + [f"{g}{p}{s}{j}" for g in ("", "g") for p in "YZ" for s in "+-" for j in (1, 2, 3)]
SEM = {n: i for i, n in enumerate(SEMS)}


def _dot(a, b, ca=1, cb=0):
    return lax.dot_general(a, b, (((ca,), (cb,)), ((), ())), preferred_element_type=F32)


def kernel(x_ref, ga_ref, gm_ref, wq_ref, wk_ref, wv_ref, wo_ref, wg_ref, wu_ref, wd_ref, yb_ref,
           own, oth, drx, yrs, yrr, yls, ylr, zls, zlr, zrs, zrr, och, xch, hst, ablk, wsl, acc, hid, kst, vst, seen, gain, cos_ref, sin_ref,
           ssem, rsem, cred, wsem, asem, xsem, osem):
    t = lax.axis_index("tp")
    c, z, y = lax.rem(t, 2), lax.rem(lax.div(t, 2), 4), lax.div(t, 8)

    def at(y_, z_, c_):
        return (y_ * 4 + z_) * 2 + c_

    peer = {"c": at(y, z, 1 - c), "y": at(1 - y, z, c), "+": at(y, jnp.minimum(z + 1, 3), c), "-": at(y, jnp.maximum(z - 1, 0), c)}

    def signal(sem, to):
        pl.semaphore_signal(sem, inc=1, device_id={"tp": peer[to]}, device_id_type=pl.DeviceIdType.MESH)

    def each_peer(fn):
        fn("c")
        fn("y")
        pl.when(z > 0)(lambda: fn("-"))
        pl.when(z < 3)(lambda: fn("+"))

    barrier = pltpu.get_barrier_semaphore()
    each_peer(lambda p: signal(barrier, p))
    pl.when((z == 0) | (z == 3))(lambda: pl.semaphore_wait(barrier, 3))
    pl.when((z > 0) & (z < 3))(lambda: pl.semaphore_wait(barrier, 4))

    def rdma(name, par, src, dst, to):
        return pltpu.make_async_remote_copy(src_ref=src, dst_ref=dst, send_sem=ssem.at[SEM[name], par], recv_sem=rsem.at[SEM[name], par],
                                            device_id={"tp": peer[to]}, device_id_type=pl.DeviceIdType.MESH)

    NW = NJ * 8 + NJ * 24

    def fetch(w):
        slot = lax.rem(w, 3)
        sem = wsem.at[slot]

        def go(src, lo, n):
            pltpu.make_async_copy(src, wsl.at[slot, pl.ds(lo, n), :], sem).start()

        @pl.when(w < NJ * 8)
        def _():
            j = lax.rem(w, 8)
            h = lax.rem(j, 2)
            for n, ref in enumerate((wq_ref, wk_ref, wv_ref)):
                pl.when(lax.div(j, 2) == n)(lambda ref=ref: go(ref.at[pl.ds(h * KH, KH), :], 0, KH))

            @pl.when(j >= 6)
            def _():
                for p in range(8):
                    go(wo_ref.at[:, pl.ds(h * KH + p * PW, PW)], p * HW, HW)

        @pl.when((w >= NJ * 8) & (w < NW))
        def _():
            u = lax.rem(w - NJ * 8, 24)
            for n, ref in enumerate((wg_ref, wu_ref)):
                @pl.when((u < 16) & (lax.rem(u, 2) == n))
                def _(ref=ref):
                    for p in range(3):
                        go(ref.at[pl.ds(lax.div(u, 2) * GK, GK), pl.ds(p * PW, PW)], p * GK, GK)

            @pl.when(u >= 16)
            def _():
                for p in range(2):
                    go(wd_ref.at[:, pl.ds((u - 16) * 2 * PW + p * PW, PW)], p * FL, FL)

    def tile_wait(w, rows):
        slot = lax.rem(w, 3)
        ref = wsl.at[slot, pl.ds(0, rows), :]
        pltpu.make_async_copy(ref, ref, wsem.at[slot]).wait()
        fetch(w + 2)
        return slot

    def rows_start(job):
        slot = lax.rem(job, 2)

        def eight(q, _):
            item, u, v = lax.div(q, 16), lax.rem(lax.div(q, 4), 2), lax.rem(q, 4)

            @pl.when(job < NJ)
            def _():
                src = x_ref.at[2 * job + item, lax.rem(lax.div(q, 8), 2), u, v]
                pltpu.make_async_copy(src, ablk.at[slot, pl.ds(pl.multiple_of(q * C, C), C), :], asem.at[slot]).start()

            @pl.when(job >= NJ)
            def _():
                half = lax.rem(lax.div(q, 8), 2)
                src = yb_ref.at[2 * (job - NJ) + item, lax.rem(c + half, 2), u, v]
                at_row = pl.multiple_of(half * R + item * RH + (u * 4 + v) * C, C)
                pltpu.make_async_copy(src, ablk.at[slot, pl.ds(at_row, C), :], asem.at[slot]).start()

        pl.when(job < 2 * NJ)(lambda: lax.fori_loop(0, 32, eight, None))

    def rows_wait(job):
        slot = lax.rem(job, 2)
        pltpu.make_async_copy(ablk.at[slot], ablk.at[slot], asem.at[slot]).wait()

    def put(job, out, col):
        cols = pl.ds(pl.multiple_of(col, PW), PW)
        for q in range(2):
            own[lax.rem(2 * job + q, OS), :, :, :, cols] = out[q * RH : (q + 1) * RH].reshape(2, 4, C, PW)
            oth[lax.rem(2 * job + q, OT), :, :, :, cols] = out[R + q * RH : R + (q + 1) * RH].reshape(2, 4, C, PW).astype(BF16)

    def attention_part(job, n):
        ab = lax.rem(job, 2)
        half = lax.rem(job, 2)
        tile = jnp.where(n < 8, n - 2, 6 + lax.div(n - 10, 2))
        w = job * 8 + tile
        slot = lax.rem(jnp.maximum(w, 0), 3)

        pl.when(n == 0)(lambda: rows_wait(job))

        @pl.when(n < 2)
        def _():
            def norm(g, _):
                rows = pl.ds(pl.multiple_of(n * R + g * 16, 16), 16)
                total = jnp.zeros((16, HEAD), F32)
                for j in range(0, D, GK):
                    v = ablk[ab, rows, j : j + GK].astype(F32)
                    v = v * v
                    for q in range(0, GK, HEAD):
                        total += v[:, q : q + HEAD]
                scale = lax.rsqrt(jnp.sum(total, -1, keepdims=True) * (1 / D) + 1e-6)
                for j in range(0, D, GK):
                    v = ablk[ab, rows, j : j + GK].astype(F32) * scale
                    v = v.reshape(2, 8, GK) * gain[0, :, j : j + GK]
                    ablk[ab, rows, j : j + GK] = v.reshape(16, GK).astype(BF16)

            lax.fori_loop(0, R // 16, norm, None)

        @pl.when(n == 1)
        def _():
            acc[0] = jnp.zeros((JR, FL), F32)

        @pl.when(((n >= 2) & (n < 8)) | (n == 10) | (n == 12))
        def _():
            tile_wait(w, KH)

        @pl.when((n >= 2) & (n < 8))
        def _():
            cols = pl.ds(pl.multiple_of(lax.div(tile, 2) * PW, PW), PW)
            lhs = ablk[ab, :, pl.ds(pl.multiple_of(lax.rem(tile, 2) * KH, KH), KH)]
            acc[0, :, cols] += _dot(lhs, wsl[slot])

        @pl.when((n == 8) | (n == 9))
        def _():
            place = pl.ds(pl.multiple_of(half * JR, JR), JR)

            def head(i, _):
                cos, sin = cos_ref[place, :], sin_ref[place, :]

                def column(first):
                    return acc[0, :, pl.ds(pl.multiple_of(first + i * HEAD, HEAD), HEAD)].astype(BF16)

                def turn(first):
                    v = column(first).astype(F32)
                    return (v * cos + pltpu.roll(v, HEAD // 2, 1) * sin).astype(BF16)

                q = turn(0)
                kst[i, place, :] = turn(PW)
                vst[i, place, :] = column(2 * PW)

                def attend(seen_keys):
                    s = _dot(q, kst[i, :seen_keys, :], 1, 1) * HEAD**-0.5
                    token = lax.broadcasted_iota(jnp.int32, s.shape, 0) + (seen_keys - JR)
                    s = jnp.where(token >= lax.broadcasted_iota(jnp.int32, s.shape, 1), s, -1e30)
                    p = jnp.exp(s - s.max(-1, keepdims=True))
                    p = (p * (1 / p.sum(-1, keepdims=True))).astype(BF16)
                    o = _dot(p, vst[i, :seen_keys, :]).astype(BF16)
                    cols = pl.ds(pl.multiple_of(i * HEAD, HEAD), HEAD)
                    for h in range(4):
                        at_row = lax.rem(c + h, 2) * R + (h // 2) * RH
                        seen[pl.ds(pl.multiple_of(at_row, RH), RH), cols] = o[h * RH : (h + 1) * RH]

                pl.when(half == 0)(lambda: attend(JR))
                pl.when(half == 1)(lambda: attend(2 * JR))

            lax.fori_loop((n - 8) * 2, (n - 8) * 2 + 2, head, None)

        @pl.when(n >= 10)
        def _():
            for p in range(4):
                q = lax.rem(n, 2) * 4 + p
                put(job, _dot(seen[...], wsl[slot, pl.ds(pl.multiple_of(q * HW, HW), HW), :]), (tile - 6) * KH + q * PW)

    def mlp_part(job, u):
        ab = lax.rem(job, 2)

        @pl.when(u == 0)
        def _():
            rows_wait(job)
            acc[...] = jnp.zeros((2, JR, FL), F32)

        slot = tile_wait(NJ * 8 + (job - NJ) * 24 + u, 3 * GK)

        @pl.when(u < 16)
        def _():
            lhs = ablk[ab, :, pl.ds(pl.multiple_of(lax.div(u, 2) * GK, GK), GK)]
            which = lax.rem(u, 2)
            for p in range(3):
                acc[which, :, p * PW : (p + 1) * PW] += _dot(lhs, wsl[slot, p * GK : (p + 1) * GK, :])

        @pl.when(u == 15)
        def _():
            def rows(g, _):
                r = pl.ds(pl.multiple_of(g * 16, 16), 16)
                gate = acc[0, r, :]
                hid[r, :] = (gate * (1 / (1 + jnp.exp(-gate))) * acc[1, r, :]).astype(BF16)

            lax.fori_loop(0, JR // 16, rows, None)

        @pl.when(u >= 16)
        def _():
            for p in range(2):
                put(job, _dot(hid[...], wsl[slot, p * FL : (p + 1) * FL, :]), (u - 16) * 2 * PW + p * PW)

    def rs_send(s, j):
        return ((z < 3) & (j > z), 4 + z - j) if s == "+" else ((z > 0) & (j >= 4 - z), j + z - 4)

    def rs_recv(s, j):
        return (z >= 1) & (j >= z) if s == "+" else (z <= 2) & (j >= 3 - z)

    def first(s):
        return z == 0 if s == "+" else z == 3

    def ag_send(s, j):
        return ((z < 3) & (j <= z + 1), z - (j - 1)) if s == "+" else ((z > 0) & (j <= 4 - z), z + (j - 1))

    def ag_recv(s, j):
        return ((z >= 1) & (j <= z), z - j) if s == "+" else ((z <= 2) & (j <= 3 - z), z + j)

    YC, ZC = pl.ds(0, CY), pl.ds(CY, CZ)
    S = {"+": 0, "-": 1}

    def core(i, par):
        return rdma("D", par, oth.at[lax.rem(i, OT)], drx.at[par], "c")

    def sd(i, par):
        @pl.when(par == 0)
        def _():
            for q in range(2):
                core(i + q, q).start()

    def y_line(i, par, j):
        for s in "+-":
            yes, k = rs_send(s, j)

            @pl.when(yes & first(s))
            def _():
                yls[S[s], j - 1] = own[lax.rem(i, OS), y, k, :, YC].astype(BF16)

            if j > 1:
                @pl.when(yes & ~first(s))
                def _():
                    yls[S[s], j - 1] = (own[lax.rem(i, OS), y, k, :, YC] + ylr[par, S[s], j - 2].astype(F32)).astype(BF16)

            pl.when(yes)(rdma(f"Y{s}{j}", par, yls.at[S[s], j - 1], ylr.at[par, S[s], j - 1], s).start)

    def z_line(i, par, j):
        for s in "+-":
            yes, k = rs_send(s, j)

            @pl.when(yes & first(s))
            def _():
                for h in range(2):
                    zls[S[s], j - 1, h] = own[lax.rem(i, OS), h, k, :, ZC].astype(BF16)

            if j > 1:
                @pl.when(yes & ~first(s))
                def _():
                    for h in range(2):
                        zls[S[s], j - 1, h] = (own[lax.rem(i, OS), h, k, :, ZC] + zlr[par, S[s], j - 2, h].astype(F32)).astype(BF16)

            pl.when(yes)(rdma(f"Z{s}{j}", par, zls.at[S[s], j - 1], zlr.at[par, S[s], j - 1], s).start)

    def line_wait(part, par, j):
        sb, rb = (yls, ylr) if part == "Y" else (zls, zlr)
        for s in "+-":
            cp = rdma(f"{part}{s}{j}", par, sb.at[S[s], j - 1], rb.at[par, S[s], j - 1], s)
            pl.when(rs_send(s, j)[0])(cp.wait_send)
            pl.when(rs_recv(s, j))(cp.wait_recv)

    def s0(i, par):
        core(i, par).wait_recv()
        pl.when(par == 0)(core(i, 0).wait_send)
        slot = lax.rem(i, OS)

        def add(k, _):
            a, b = lax.div(k, 4), lax.rem(k, 4)
            own[slot, a, b] += drx[par, a, b].astype(F32)

        lax.fori_loop(0, 8, add, None)

        def cast(k, _):
            yrs[k] = own[slot, 1 - y, k, :, YC].astype(BF16)

        lax.fori_loop(0, 4, cast, None)
        rdma("YR", par, yrs, yrr.at[par], "y").start()
        z_line(i, par, 1)

    def s1(i, par):
        pl.when(par == 0)(core(i, 1).wait_send)
        rdma("YR", par, yrs, yrr.at[par], "y").wait()
        slot = lax.rem(i, OS)

        def add(k, _):
            own[slot, y, k, :, YC] += yrr[par, k].astype(F32)

        lax.fori_loop(0, 4, add, None)
        y_line(i, par, 1)
        line_wait("Z", par, 1)
        z_line(i, par, 2)

    def s2(i, par):
        line_wait("Y", par, 1)
        y_line(i, par, 2)
        line_wait("Z", par, 2)
        z_line(i, par, 3)

    def x_copy(i):
        return pltpu.make_async_copy(x_ref.at[i, c, y, z], xch, xsem)

    def s3(i, par):
        pl.when(i < NI)(lambda: x_copy(i).start())
        line_wait("Y", par, 2)
        y_line(i, par, 3)
        line_wait("Z", par, 3)
        slot = lax.rem(i, OS)
        for s in "+-":
            @pl.when(rs_recv(s, 3))
            def _():
                for h in range(2):
                    own[slot, h, z, :, ZC] += zlr[par, S[s], 2, h].astype(F32)
        zrs[...] = own[slot, 1 - y, z, :, ZC].astype(BF16)
        rdma("ZR", par, zrs, zrr.at[par], "y").start()

    def och_copy(i):
        return pltpu.make_async_copy(och, yb_ref.at[i, c, y, z], osem)

    def ag_first(i, par):
        cps = [(ag_send(s, 1)[0], ag_recv(s, 1)[0], rdma(f"gY{s}1", par, och.at[:, YC], yb_ref.at[i, c, y, z, :, YC], s)) for s in "+-"]
        return cps, rdma("gZR", par, och.at[:, ZC], yb_ref.at[i, c, y, z, :, ZC], "y")

    def s4(i, par):
        slot = lax.rem(i, OS)
        line_wait("Y", par, 3)
        for s in "+-":
            @pl.when(rs_recv(s, 3))
            def _():
                own[slot, y, z, :, YC] += ylr[par, S[s], 2].astype(F32)
        rdma("ZR", par, zrs, zrr.at[par], "y").wait()
        own[slot, y, z, :, ZC] += zrr[par].astype(F32)

        @pl.when(i < NI)
        def _():
            x_copy(i).wait()
            h = (xch[...].astype(F32) + own[slot, y, z]).astype(BF16)
            hst[i] = h
            v = h.astype(F32)
            scale = lax.rsqrt(jnp.mean(v * v, -1, keepdims=True) + 1e-6)
            och[...] = (v * scale * gain[1]).astype(BF16)

        @pl.when(i >= NI)
        def _():
            och[...] = (hst[i - NI].astype(F32) + own[slot, y, z]).astype(BF16)

        och_copy(i).start()
        lines, rung = ag_first(i, par)
        for yes, _, cp in lines:
            pl.when(yes)(cp.start)
        rung.start()

    def ag_y(i, par, j):
        return [(*ag_send(s, j), *ag_recv(s, j), s) for s in "+-"]

    def g_src(part, i, k):
        return yb_ref.at[i, c, y, k, :, YC] if part == "Y" else yb_ref.at[i, c, :, k, :, ZC]

    def g_line(part, i, par, j):
        for s in "+-":
            yes, k = ag_send(s, j)

            @pl.when(yes)
            def _():
                rdma(f"g{part}{s}{j}", par, g_src(part, i, k), g_src(part, i, k), s).start()

    def g_wait(part, i, par, j):
        for s in "+-":
            yes, k = ag_send(s, j)
            got, _ = ag_recv(s, j)
            ref = g_src(part, i, 0)
            cp = rdma(f"g{part}{s}{j}", par, ref, ref, s)
            pl.when(yes)(cp.wait_send)
            pl.when(got)(cp.wait_recv)

    def s5(i, par):
        och_copy(i).wait()
        lines, rung = ag_first(i, par)
        for yes, got, cp in lines:
            pl.when(yes)(cp.wait_send)
            pl.when(got)(cp.wait_recv)
        g_line("Y", i, par, 2)
        rung.wait()
        g_line("Z", i, par, 1)

    def s6(i, par):
        g_wait("Y", i, par, 2)
        g_line("Y", i, par, 3)
        g_wait("Z", i, par, 1)
        g_line("Z", i, par, 2)

    def g_rung(i, par):
        ref = yb_ref.at[i, c, y, :, :, YC]
        return rdma("gYR", par, ref, ref, "y")

    def g_core(i, par):
        ref = yb_ref.at[i, c]
        return rdma("gD", par, ref, ref, "c")

    def s7(i, par):
        g_wait("Y", i, par, 3)
        g_rung(i, par).start()
        g_wait("Z", i, par, 2)
        g_line("Z", i, par, 3)

    def s8(i, par):
        g_rung(i, par).wait()
        g_wait("Z", i, par, 3)
        g_core(i, par).start()

    def s9(i, par):
        g_core(i, par).wait()

    actions = [("sd", sd), ("s0", s0), ("s1", s1), ("s2", s2), ("s3", s3), ("s4", s4), ("s5", s5), ("s6", s6), ("s7", s7), ("s8", s8), ("s9", s9)]
    order = sorted(actions, key=lambda a: -AT[a[0]][0])

    CR = {"c": 0, "y": 1, "-": 2, "+": 3}
    BACK = {"c": 0, "y": 1, "-": 3, "+": 2}

    rows_start(0)
    fetch(0)
    fetch(1)
    for n, ref in enumerate((ga_ref, gm_ref)):
        for q in range(D // HEAD):
            gain[n, :, q * HEAD : (q + 1) * HEAD] = jnp.broadcast_to(ref[q : q + 1, :].astype(F32), (8, HEAD))

    def turns(g, _):
        shape = (64, HEAD)
        lane = lax.broadcasted_iota(jnp.int32, shape, 1)
        place = (lax.broadcasted_iota(jnp.int32, shape, 0) + g * 64).astype(F32)
        angle = place * jnp.exp(lax.rem(lane, HEAD // 2).astype(F32) * (-math.log(THETA) / (HEAD // 2)))
        rows = pl.ds(pl.multiple_of(g * 64, 64), 64)
        cos_ref[rows, :] = jnp.cos(angle)
        sin_ref[rows, :] = jnp.where(lane < HEAD // 2, -1.0, 1.0) * jnp.sin(angle)

    lax.fori_loop(0, 2 * JR // 64, turns, None)

    def parts_by(m):
        return jnp.minimum(m, 14 * NJ) + jnp.minimum(lax.div(jnp.maximum(m - 14 * NJ, 0) * 15, 11), 24 * NJ)

    def compute(n, _):
        @pl.when(n < 14 * NJ)
        def _():
            job, part = lax.div(n, 14), lax.rem(n, 14)
            pl.when(part == 4)(lambda: rows_start(job + 1))
            attention_part(job, part)

        @pl.when(n >= 14 * NJ)
        def _():
            job, part = NJ + lax.div(n - 14 * NJ, 24), lax.rem(n - 14 * NJ, 24)
            pl.when(part == 6)(lambda: rows_start(job + 1))
            mlp_part(job, part)

    def body(m, _):
        k, n = lax.div(m + 2, NS) - 2, lax.rem(m + 2, NS)
        pl.when((n == 0) & (k >= 1))(lambda: each_peer(lambda p: pl.semaphore_wait(cred.at[CR[p]], 1)))
        for name, fn in order:
            d, pos = AT[name]
            i = k - d
            pl.when((n == pos) & (i >= 0) & (i < NT))(lambda fn=fn, i=i: fn(i, lax.rem(i, 2)))
        lax.fori_loop(parts_by(m), parts_by(m + 1), compute, None)
        pl.when((n == 5) & (k >= 0) & (k < LAST))(lambda: each_peer(lambda p: signal(cred.at[BACK[p]], p)))

    lax.fori_loop(0, (LAST + 3) * NS - 2, body, None)


def solution(mesh):
    def step(x, gain_a, wq, wk, wv, wo, gain_m, w_gate, w_up, w_down):
        batch, rows, d = x.shape
        hbm, vmem = pl.BlockSpec(memory_space=pl.ANY), pl.BlockSpec(memory_space=pltpu.VMEM)
        yb = pl.pallas_call(
            kernel,
            out_shape=jax.ShapeDtypeStruct((NT, 2, 2, 4, C, D), BF16),
            in_specs=[hbm, vmem, vmem] + [hbm] * 7,
            out_specs=hbm,
            scratch_shapes=[
                pltpu.VMEM((OS, 2, 4, C, D), F32),
                pltpu.VMEM((OT, 2, 4, C, D), BF16),
                pltpu.VMEM((2, 2, 4, C, D), BF16),
                pltpu.VMEM((4, C, CY), BF16),
                pltpu.VMEM((2, 4, C, CY), BF16),
                pltpu.VMEM((2, 3, C, CY), BF16),
                pltpu.VMEM((2, 2, 3, C, CY), BF16),
                pltpu.VMEM((2, 3, 2, C, CZ), BF16),
                pltpu.VMEM((2, 2, 3, 2, C, CZ), BF16),
                pltpu.VMEM((C, CZ), BF16),
                pltpu.VMEM((2, C, CZ), BF16),
                pltpu.VMEM((C, D), BF16),
                pltpu.VMEM((C, D), BF16),
                pltpu.VMEM((NI, C, D), BF16),
                pltpu.VMEM((2, JR, D), BF16),
                pltpu.VMEM((3, KH, PW), BF16),
                pltpu.VMEM((2, JR, FL), F32),
                pltpu.VMEM((JR, FL), BF16),
                pltpu.VMEM((HW // HEAD, 2 * JR, HEAD), BF16),
                pltpu.VMEM((HW // HEAD, 2 * JR, HEAD), BF16),
                pltpu.VMEM((JR, HW), BF16),
                pltpu.VMEM((2, 8, D), F32),
                pltpu.VMEM((2 * JR, HEAD), F32),
                pltpu.VMEM((2 * JR, HEAD), F32),
                pltpu.SemaphoreType.DMA((len(SEMS), 2)),
                pltpu.SemaphoreType.DMA((len(SEMS), 2)),
                pltpu.SemaphoreType.REGULAR((4,)),
                pltpu.SemaphoreType.DMA((3,)),
                pltpu.SemaphoreType.DMA((2,)),
                pltpu.SemaphoreType.DMA,
                pltpu.SemaphoreType.DMA,
            ],
            compiler_params=pltpu.CompilerParams(collective_id=0, has_side_effects=True, vmem_limit_bytes=67043328),
            name="layer",
        )(x.reshape(NI, 2, 2, 4, C, D), gain_a.reshape(-1, HEAD), gain_m.reshape(-1, HEAD), wq, wk, wv, wo, w_gate, w_up, w_down)
        return yb[NI:].reshape(x.shape)

    tokens, whole, columns, rows_of = P("dp", None, None), P(None), P(None, "tp"), P("tp", None)
    return jax.shard_map(
        step,
        mesh=mesh,
        in_specs=(tokens, whole, columns, columns, columns, rows_of, whole, columns, columns, rows_of),
        out_specs=tokens,
        check_vma=False,
    )
```

```python
import functools
import math

import jax
import jax.numpy as jnp
from jax import lax
from jax.experimental import pallas as pl
from jax.experimental.pallas import tpu as pltpu
from jax.sharding import PartitionSpec as P

HEAD = 128
THETA = 10000
F32, BF16 = jnp.float32, jnp.bfloat16

JR = 256
R = JR // 2
RH = R // 2
C = RH // 8
NJ = 8
NI = 2 * NJ
NT = 2 * NI
OS = 7
OT = 4
WS = 4
MP = 13
NP = 9
AT_MLP = 100
D, HW, FL = 8192, 512, 1536
CY = 4864
CZ = D - CY
KH, GK, PW = D // 2, 1024, 512
NS = 8
AT = {"sd": (0, 0), "s0": (0, 1), "s1": (0, 6), "s2": (1, 2), "s3": (1, 7), "s4": (2, 3), "s5": (3, 0), "s6": (3, 4), "s7": (4, 1), "s8": (4, 5), "s9": (4, 7)}
LAST = NT - 1 + AT["s9"][0]

SEMS = ["D", "ZR", "gZR", "gD", "gR0"] + [f"YR{q}" for q in range(4)] + [f"gR{s}{j}" for s in "+-" for j in (1, 2, 3)] + [f"{g}{p}{s}{j}" for g in ("", "g") for p in "YZ" for s in "+-" for j in (1, 2, 3)]
SEM = {n: i for i, n in enumerate(SEMS)}


def _dot(a, b, ca=1, cb=0):
    return lax.dot_general(a, b, (((ca,), (cb,)), ((), ())), preferred_element_type=F32)


def kernel(x_ref, xj_ref, ga_ref, gm_ref, wq_ref, wk_ref, wv_ref, wo_ref, wg_ref, wu_ref, wd_ref, yb_ref,
           own, oth, drx, yrs, yrr, yls, ylr, zls, zlr, zrs, zrr, och, xch, hst, ablk, wsl, acc, hid, kst, vst, seen, gain, cos_ref, sin_ref,
           ssem, rsem, cred, wsem, asem, xsem, osem):
    t = lax.axis_index("tp")
    c, z, y = lax.rem(t, 2), lax.rem(lax.div(t, 2), 4), lax.div(t, 8)

    def at(y_, z_, c_):
        return (y_ * 4 + z_) * 2 + c_

    peer = {"c": at(y, z, 1 - c), "y": at(1 - y, z, c), "+": at(y, jnp.minimum(z + 1, 3), c), "-": at(y, jnp.maximum(z - 1, 0), c)}

    def signal(sem, to):
        pl.semaphore_signal(sem, inc=1, device_id={"tp": peer[to]}, device_id_type=pl.DeviceIdType.MESH)

    def each_peer(fn):
        fn("c")
        fn("y")
        pl.when(z > 0)(lambda: fn("-"))
        pl.when(z < 3)(lambda: fn("+"))

    barrier = pltpu.get_barrier_semaphore()
    each_peer(lambda p: signal(barrier, p))
    pl.when((z == 0) | (z == 3))(lambda: pl.semaphore_wait(barrier, 3))
    pl.when((z > 0) & (z < 3))(lambda: pl.semaphore_wait(barrier, 4))

    def rdma(name, par, src, dst, to):
        return pltpu.make_async_remote_copy(src_ref=src, dst_ref=dst, send_sem=ssem.at[SEM[name], par], recv_sem=rsem.at[SEM[name], par],
                                            device_id={"tp": peer[to]}, device_id_type=pl.DeviceIdType.MESH)

    NA = (NJ + 1) * 8
    NW = NA + NJ * 24

    def fetch(w):
        slot = lax.rem(w, WS)
        sem = wsem.at[slot]

        def go(src, lo, n):
            pltpu.make_async_copy(src, wsl.at[slot, pl.ds(lo, n), :], sem).start()

        @pl.when(w < NA)
        def _():
            j = lax.rem(w, 8)
            h = lax.rem(j, 2)
            for n, ref in enumerate((wq_ref, wk_ref, wv_ref)):
                pl.when(lax.div(j, 2) == n)(lambda ref=ref: go(ref.at[pl.ds(h * KH, KH), :], 0, KH))

            @pl.when(j >= 6)
            def _():
                for p in range(8):
                    go(wo_ref.at[:, pl.ds(h * KH + p * PW, PW)], p * HW, HW)

        @pl.when((w >= NA) & (w < NW))
        def _():
            u = lax.rem(w - NA, 24)
            for n, ref in enumerate((wg_ref, wu_ref)):
                @pl.when((u < 16) & (lax.rem(u, 2) == n))
                def _(ref=ref):
                    for p in range(3):
                        go(ref.at[pl.ds(lax.div(u, 2) * GK, GK), pl.ds(p * PW, PW)], p * GK, GK)

            @pl.when(u >= 16)
            def _():
                for p in range(2):
                    go(wd_ref.at[:, pl.ds((u - 16) * 2 * PW + p * PW, PW)], p * FL, FL)

    def tile_wait(w, rows):
        slot = lax.rem(w, WS)
        ref = wsl.at[slot, pl.ds(0, rows), :]
        pltpu.make_async_copy(ref, ref, wsem.at[slot]).wait()
        return slot

    def rows_start(job):
        slot = lax.rem(job, 2)

        def eight(q, _):
            item, u, v = lax.div(q, 16), lax.rem(lax.div(q, 4), 2), lax.rem(q, 4)

            half = lax.rem(lax.div(q, 8), 2)
            src = yb_ref.at[2 * (job - NJ) + item, lax.rem(c + half, 2), u, v]
            at_row = pl.multiple_of(half * R + item * RH + (u * 4 + v) * C, C)
            pltpu.make_async_copy(src, ablk.at[slot, pl.ds(at_row, C), :], asem.at[slot]).start()

        pl.when(job < NJ)(pltpu.make_async_copy(xj_ref.at[jnp.minimum(job, NJ - 1)], ablk.at[slot], asem.at[slot]).start)
        pl.when((job >= NJ) & (job < 2 * NJ))(lambda: lax.fori_loop(0, 32, eight, None))

    def rows_wait(job):
        slot = lax.rem(job, 2)
        pltpu.make_async_copy(ablk.at[slot], ablk.at[slot], asem.at[slot]).wait()

    def put(item, out, col):
        cols = pl.ds(pl.multiple_of(col, PW), PW)
        n = out.shape[0] // R
        for q in range(n):
            own[lax.rem(item + q, OS), :, :, :, cols] = out[q * RH : (q + 1) * RH].reshape(2, 4, C, PW)
            oth[lax.rem(item + q, OT), :, :, :, cols] = out[(n + q) * RH : (n + q + 1) * RH].reshape(2, 4, C, PW).astype(BF16)

    def attention_part(step, n, size):
        job = jnp.maximum(step - 1, 0)
        item = step if size == R else 2 * job
        at_row = step * R if size == R else 0
        mine = pl.ds(pl.multiple_of(at_row, R), size)
        ab = lax.rem(job, 2)
        half = lax.rem(job, 2)
        w = step * 8

        pl.when((n == 0) & (step != 1))(lambda: rows_wait(job))

        @pl.when((n == 0) & (step == 0))
        def _():
            for q in range(2, WS):
                fetch(q)

        @pl.when(n < size // R)
        def _():
            def norm(g, _):
                rows = pl.ds(pl.multiple_of(at_row + n * R + g * 32, 32), 32)
                total = jnp.zeros((32, HEAD), F32)
                for j in range(0, D, GK):
                    v = ablk[ab, rows, j : j + GK].astype(F32)
                    v = v * v
                    for q in range(0, GK, HEAD):
                        total += v[:, q : q + HEAD]
                scale = lax.rsqrt(jnp.sum(total, -1, keepdims=True) * (1 / D) + 1e-6)
                for j in range(0, D, GK):
                    v = ablk[ab, rows, j : j + GK].astype(F32) * scale
                    v = v.reshape(4, 8, GK) * gain[0, :, j : j + GK]
                    ablk[ab, rows, j : j + GK] = v.reshape(32, GK).astype(BF16)

            lax.fori_loop(0, R // 32, norm, None)

        @pl.when((n >= 2) & (n < 5))
        def _():
            tile = w + (n - 2) * 2
            slots = [tile_wait(tile + q, KH) for q in range(2)]
            cols = pl.ds(pl.multiple_of((n - 2) * PW, PW), PW)
            acc[0, mine, cols] = _dot(ablk[ab, mine, :KH], wsl[slots[0]]) + _dot(ablk[ab, mine, KH:], wsl[slots[1]])
            for q in range(2):
                fetch(tile + q + WS)

        @pl.when((n == 5) | (n == 6))
        def _():
            first = (n - 5) * 2
            col = pl.multiple_of(first * HEAD, 2 * HEAD)
            place = pl.ds(pl.multiple_of(half * JR + at_row, R), size)
            cos, sin = cos_ref[place, :], sin_ref[place, :]

            def column(at_col, i):
                return acc[0, mine, pl.ds(pl.multiple_of(at_col + col + i * HEAD, HEAD), HEAD)].astype(BF16)

            def turn(at_col, i):
                v = column(at_col, i).astype(F32)
                return (v * cos + pltpu.roll(v, HEAD // 2, 1) * sin).astype(BF16)

            qs = [turn(0, i) for i in range(2)]
            for i in range(2):
                kst[first + i, place, :] = turn(PW, i)
                vst[first + i, place, :] = column(2 * PW, i)

            def attend(seen_keys):
                for i in range(2):
                    s = _dot(qs[i], kst[first + i, :seen_keys, :], 1, 1) * HEAD**-0.5
                    token = lax.broadcasted_iota(jnp.int32, s.shape, 0) + (seen_keys - size)
                    s = jnp.where(token >= lax.broadcasted_iota(jnp.int32, s.shape, 1), s, -1e30)
                    p = jnp.exp(s - s.max(-1, keepdims=True))
                    p = (p * (1 / p.sum(-1, keepdims=True))).astype(BF16)
                    o = _dot(p, vst[first + i, :seen_keys, :]).astype(BF16)
                    for h in range(size // RH):
                        to_row = lax.rem(c + h, 2) * (size // 2) + (h // 2) * RH
                        seen[pl.ds(pl.multiple_of(to_row, RH), RH), pl.ds(pl.multiple_of(col + i * HEAD, HEAD), HEAD)] = o[h * RH : (h + 1) * RH]

            early = step == 0 if size == R else half == 0
            pl.when(early)(lambda: attend(size))
            pl.when(~early)(lambda: attend(2 * size))

        @pl.when(n >= 7)
        def _():
            tile = w + n - 1
            slot = tile_wait(tile, KH)
            for p in range(8):
                put(item, _dot(seen[:size], wsl[slot, p * HW : (p + 1) * HW, :]), (n - 7) * KH + p * PW)
            fetch(tile + WS)

    def mlp_part(job, u):
        ab = lax.rem(job, 2)
        w = NA + (job - NJ) * 24 + 2 * jnp.where(u < 8, u, u - 1)

        @pl.when(u == 0)
        def _():
            rows_wait(job)
            acc[...] = jnp.zeros((2, JR, FL), F32)

        @pl.when(u < 8)
        def _():
            slots = [tile_wait(w + q, 3 * GK) for q in range(2)]
            lhs = ablk[ab, :, pl.ds(pl.multiple_of(u * GK, GK), GK)]
            for q in range(2):
                for p in range(3):
                    acc[q, :, p * PW : (p + 1) * PW] += _dot(lhs, wsl[slots[q], p * GK : (p + 1) * GK, :])
            for q in range(2):
                fetch(w + q + WS)

        @pl.when(u == 8)
        def _():
            def rows(g, _):
                r = pl.ds(pl.multiple_of(g * 16, 16), 16)
                gate = acc[0, r, :]
                hid[r, :] = (gate * (1 / (1 + jnp.exp(-gate))) * acc[1, r, :]).astype(BF16)

            lax.fori_loop(0, JR // 16, rows, None)

        @pl.when(u > 8)
        def _():
            slots = [tile_wait(w + q, 3 * GK) for q in range(2)]
            for q in range(2):
                for p in range(2):
                    put(2 * job, _dot(hid[...], wsl[slots[q], p * FL : (p + 1) * FL, :]), ((u - 9) * 2 + q) * 2 * PW + p * PW)
            for q in range(2):
                fetch(w + q + WS)

    def rs_send(s, j):
        return ((z < 3) & (j > z), 4 + z - j) if s == "+" else ((z > 0) & (j >= 4 - z), j + z - 4)

    def rs_recv(s, j):
        return (z >= 1) & (j >= z) if s == "+" else (z <= 2) & (j >= 3 - z)

    def first(s):
        return z == 0 if s == "+" else z == 3

    def ag_send(s, j):
        return ((z < 3) & (j <= z + 1), z - (j - 1)) if s == "+" else ((z > 0) & (j <= 4 - z), z + (j - 1))

    def ag_recv(s, j):
        return ((z >= 1) & (j <= z), z - j) if s == "+" else ((z <= 2) & (j <= 3 - z), z + j)

    YC, ZC = pl.ds(0, CY), pl.ds(CY, CZ)
    S = {"+": 0, "-": 1}

    def core(i, par):
        return rdma("D", par, oth.at[lax.rem(i, OT)], drx.at[par], "c")

    def sd(i, par):
        pl.when((i < 2) | (par == 0))(core(i, par).start)
        pl.when((i >= 2) & (par == 0))(core(i + 1, 1).start)

    def y_line(i, par, j):
        for s in "+-":
            yes, k = rs_send(s, j)

            @pl.when(yes & first(s))
            def _():
                yls[S[s], j - 1] = own[lax.rem(i, OS), y, k, :, YC].astype(BF16)

            if j > 1:
                @pl.when(yes & ~first(s))
                def _():
                    yls[S[s], j - 1] = (own[lax.rem(i, OS), y, k, :, YC] + ylr[par, S[s], j - 2].astype(F32)).astype(BF16)

            pl.when(yes)(rdma(f"Y{s}{j}", par, yls.at[S[s], j - 1], ylr.at[par, S[s], j - 1], s).start)

    def z_line(i, par, j):
        for s in "+-":
            yes, k = rs_send(s, j)

            @pl.when(yes & first(s))
            def _():
                for h in range(2):
                    zls[S[s], j - 1, h] = own[lax.rem(i, OS), h, k, :, ZC].astype(BF16)

            if j > 1:
                @pl.when(yes & ~first(s))
                def _():
                    for h in range(2):
                        zls[S[s], j - 1, h] = (own[lax.rem(i, OS), h, k, :, ZC] + zlr[par, S[s], j - 2, h].astype(F32)).astype(BF16)

            pl.when(yes)(rdma(f"Z{s}{j}", par, zls.at[S[s], j - 1], zlr.at[par, S[s], j - 1], s).start)

    def line_wait(part, par, j):
        sb, rb = (yls, ylr) if part == "Y" else (zls, zlr)
        for s in "+-":
            cp = rdma(f"{part}{s}{j}", par, sb.at[S[s], j - 1], rb.at[par, S[s], j - 1], s)
            pl.when(rs_send(s, j)[0])(cp.wait_send)
            pl.when(rs_recv(s, j))(cp.wait_recv)

    def piece(q):
        return (jnp.where(z < 2, 3, 0), jnp.where(z < 2, 2, 1), jnp.where(z < 2, 1 - z, 5 - z), z)[q]

    def rung(i, par, q):
        four = lax.rem(i, 4)
        return rdma(f"YR{q}", four, yrs.at[par, q], yrr.at[four, q], "y")

    def rung_add(i, par, q):
        rung(i, par, q).wait_recv()
        own[lax.rem(i, OS), y, piece(q), :, YC] += yrr[lax.rem(i, 4), q].astype(F32)

    def s0(i, par):
        core(i, par).wait()
        slot = lax.rem(i, OS)

        def add(k, _):
            a, b = lax.div(k, 4), lax.rem(k, 4)
            own[slot, a, b] += drx[par, a, b].astype(F32)

        lax.fori_loop(0, 8, add, None)

        for q in range(4):
            yrs[par, q] = own[slot, 1 - y, piece(q), :, YC].astype(BF16)
            rung(i, par, q).start()
            if q == 0:
                z_line(i, par, 1)

    def s1(i, par):
        rung_add(i, par, 0)
        y_line(i, par, 1)
        line_wait("Z", par, 1)
        z_line(i, par, 2)

    def s2(i, par):
        for q in range(4):
            rung(i, par, q).wait_send()
        rung_add(i, par, 1)
        line_wait("Y", par, 1)
        y_line(i, par, 2)
        line_wait("Z", par, 2)
        z_line(i, par, 3)

    def x_copy(i):
        return pltpu.make_async_copy(x_ref.at[i, c, y, z], xch, xsem)

    def s3(i, par):
        pl.when(i < NI)(lambda: x_copy(i).start())
        rung_add(i, par, 2)
        line_wait("Y", par, 2)
        y_line(i, par, 3)
        line_wait("Z", par, 3)
        slot = lax.rem(i, OS)
        for s in "+-":
            @pl.when(rs_recv(s, 3))
            def _():
                for h in range(2):
                    own[slot, h, z, :, ZC] += zlr[par, S[s], 2, h].astype(F32)
        zrs[...] = own[slot, 1 - y, z, :, ZC].astype(BF16)
        rdma("ZR", par, zrs, zrr.at[par], "y").start()

    def och_copy(i):
        return pltpu.make_async_copy(och, yb_ref.at[i, c, y, z], osem)

    def ag_first(i, par):
        cps = [(ag_send(s, 1)[0], ag_recv(s, 1)[0], rdma(f"gY{s}1", par, och.at[:, YC], yb_ref.at[i, c, y, z, :, YC], s)) for s in "+-"]
        return cps, rdma("gZR", par, och.at[:, ZC], yb_ref.at[i, c, y, z, :, ZC], "y")

    def s4(i, par):
        slot = lax.rem(i, OS)
        rung_add(i, par, 3)
        line_wait("Y", par, 3)
        for s in "+-":
            @pl.when(rs_recv(s, 3))
            def _():
                own[slot, y, z, :, YC] += ylr[par, S[s], 2].astype(F32)
        rdma("ZR", par, zrs, zrr.at[par], "y").wait()
        own[slot, y, z, :, ZC] += zrr[par].astype(F32)

        @pl.when(i < NI)
        def _():
            x_copy(i).wait()
            h = (xch[...].astype(F32) + own[slot, y, z]).astype(BF16)
            hst[i] = h
            v = h.astype(F32)
            scale = lax.rsqrt(jnp.mean(v * v, -1, keepdims=True) + 1e-6)
            och[...] = (v * scale * gain[1]).astype(BF16)

        @pl.when(i >= NI)
        def _():
            och[...] = (hst[i - NI].astype(F32) + own[slot, y, z]).astype(BF16)

        och_copy(i).start()
        lines, rung = ag_first(i, par)
        for yes, _, cp in lines:
            pl.when(yes)(cp.start)
        g_rung(i, "0").start()
        rung.start()

    def ag_y(i, par, j):
        return [(*ag_send(s, j), *ag_recv(s, j), s) for s in "+-"]

    def g_src(part, i, k):
        return yb_ref.at[i, c, y, k, :, YC] if part == "Y" else yb_ref.at[i, c, :, k, :, ZC]

    def g_line(part, i, par, j):
        for s in "+-":
            yes, k = ag_send(s, j)

            @pl.when(yes)
            def _():
                rdma(f"g{part}{s}{j}", par, g_src(part, i, k), g_src(part, i, k), s).start()

    def g_wait(part, i, par, j):
        for s in "+-":
            yes, k = ag_send(s, j)
            got, _ = ag_recv(s, j)
            ref = g_src(part, i, 0)
            cp = rdma(f"g{part}{s}{j}", par, ref, ref, s)
            pl.when(yes)(cp.wait_send)
            pl.when(got)(cp.wait_recv)

    def s5(i, par):
        och_copy(i).wait()
        lines, rung = ag_first(i, par)
        for yes, got, cp in lines:
            pl.when(yes)(cp.wait_send)
            pl.when(got)(cp.wait_recv)
        g_rung(i, "0").wait_send()
        g_line("Y", i, par, 2)
        g_rungs(i, 1)
        rung.wait()
        g_line("Z", i, par, 1)

    def s6(i, par):
        g_wait("Y", i, par, 2)
        g_line("Y", i, par, 3)
        g_rungs(i, 2)
        g_wait("Z", i, par, 1)
        g_line("Z", i, par, 2)

    def g_rung(i, name, k=0):
        ref = yb_ref.at[i, c, y, k, :, YC]
        return rdma("gR" + name, lax.rem(i, 4), och.at[:, YC] if name == "0" else ref, yb_ref.at[i, c, y, z, :, YC] if name == "0" else ref, "y")

    def g_rungs(i, j):
        for s in "+-":
            got, k = ag_recv(s, j)
            pl.when(got)(lambda: g_rung(i, f"{s}{j}", k).start())

    def g_core(i, par):
        ref = yb_ref.at[i, c]
        return rdma("gD", par, ref, ref, "c")

    def s7(i, par):
        g_wait("Y", i, par, 3)
        g_rungs(i, 3)
        g_wait("Z", i, par, 2)
        g_line("Z", i, par, 3)

    def s8(i, par):
        g_wait("Z", i, par, 3)
        g_rung(i, "0").wait_recv()
        for j in (1, 2, 3):
            for s in "+-":
                pl.when(ag_recv(s, j)[0])(lambda: g_rung(i, f"{s}{j}").wait())
        g_core(i, par).start()

    def s9(i, par):
        g_core(i, par).wait()

    actions = [("sd", sd), ("s0", s0), ("s1", s1), ("s2", s2), ("s3", s3), ("s4", s4), ("s5", s5), ("s6", s6), ("s7", s7), ("s8", s8), ("s9", s9)]
    order = sorted(actions, key=lambda a: -AT[a[0]][0])

    CR = {"c": 0, "y": 1, "-": 2, "+": 3}
    BACK = {"c": 0, "y": 1, "-": 3, "+": 2}

    rows_start(0)
    fetch(0)
    fetch(1)
    for n, ref in enumerate((ga_ref, gm_ref)):
        for q in range(D // HEAD):
            gain[n, :, q * HEAD : (q + 1) * HEAD] = jnp.broadcast_to(ref[q : q + 1, :].astype(F32), (8, HEAD))

    def turns(g, _):
        shape = (64, HEAD)
        lane = lax.broadcasted_iota(jnp.int32, shape, 1)
        place = (lax.broadcasted_iota(jnp.int32, shape, 0) + g * 64).astype(F32)
        angle = place * jnp.exp(lax.rem(lane, HEAD // 2).astype(F32) * (-math.log(THETA) / (HEAD // 2)))
        rows = pl.ds(pl.multiple_of(g * 64, 64), 64)
        cos_ref[rows, :] = jnp.cos(angle)
        sin_ref[rows, :] = jnp.where(lane < HEAD // 2, -1.0, 1.0) * jnp.sin(angle)

    lax.fori_loop(0, 2 * JR // 64, turns, None)

    def parts_by(m):
        n = jnp.maximum(m - 1, 0)

        def over(start, a, b, most):
            return jnp.minimum(lax.div(jnp.maximum(n - start, 0) * a, b), most)

        return jnp.minimum(m, 1) * NP + over(0, 9, 7, NP) + over(7, 1, 1, NP) + over(16, 9, 14, (NJ - 2) * NP) + over(AT_MLP, 16, 21, MP * NJ)

    def compute(n, _):
        ends = (NJ + 1) * NP

        @pl.when(n < ends)
        def _():
            step, part = lax.div(n, NP), lax.rem(n, NP)
            pl.when((part == 2) & (step >= 1))(lambda: rows_start(step))
            pl.when(step < 2)(lambda: attention_part(step, part, R))
            pl.when(step >= 2)(lambda: attention_part(step, part, JR))

        @pl.when(n >= ends)
        def _():
            job, part = NJ + lax.div(n - ends, MP), lax.rem(n - ends, MP)
            pl.when(part == 4)(lambda: rows_start(job + 1))
            mlp_part(job, part)

    def body(m, _):
        k, n = lax.div(m + NS - 1, NS) - 1, lax.rem(m + NS - 1, NS)
        pl.when((n == 0) & (k >= 1))(lambda: each_peer(lambda p: pl.semaphore_wait(cred.at[CR[p]], 1)))
        for name, fn in order:
            d, pos = AT[name]
            i = k - d
            pl.when((n == pos) & (i >= 0) & (i < NT))(lambda fn=fn, i=i: fn(i, lax.rem(i, 2)))
        lax.fori_loop(parts_by(m), parts_by(m + 1), compute, None)
        pl.when((n == 5) & (k >= 0) & (k < LAST))(lambda: each_peer(lambda p: signal(cred.at[BACK[p]], p)))

    lax.fori_loop(0, LAST * NS + AT["s9"][1] + 2, body, None)


def solution(mesh):
    def step(x, gain_a, wq, wk, wv, wo, gain_m, w_gate, w_up, w_down):
        batch, rows, d = x.shape
        hbm, vmem = pl.BlockSpec(memory_space=pl.ANY), pl.BlockSpec(memory_space=pltpu.VMEM)
        yb = pl.pallas_call(
            kernel,
            out_shape=jax.ShapeDtypeStruct((NT, 2, 2, 4, C, D), BF16),
            in_specs=[hbm, hbm, vmem, vmem] + [hbm] * 7,
            out_specs=hbm,
            scratch_shapes=[
                pltpu.VMEM((OS, 2, 4, C, D), F32),
                pltpu.VMEM((OT, 2, 4, C, D), BF16),
                pltpu.VMEM((2, 2, 4, C, D), BF16),
                pltpu.VMEM((2, 4, C, CY), BF16),
                pltpu.VMEM((4, 4, C, CY), BF16),
                pltpu.VMEM((2, 3, C, CY), BF16),
                pltpu.VMEM((2, 2, 3, C, CY), BF16),
                pltpu.VMEM((2, 3, 2, C, CZ), BF16),
                pltpu.VMEM((2, 2, 3, 2, C, CZ), BF16),
                pltpu.VMEM((C, CZ), BF16),
                pltpu.VMEM((2, C, CZ), BF16),
                pltpu.VMEM((C, D), BF16),
                pltpu.VMEM((C, D), BF16),
                pltpu.VMEM((NI, C, D), BF16),
                pltpu.VMEM((2, JR, D), BF16),
                pltpu.VMEM((WS, KH, PW), BF16),
                pltpu.VMEM((2, JR, FL), F32),
                pltpu.VMEM((JR, FL), BF16),
                pltpu.VMEM((HW // HEAD, 2 * JR, HEAD), BF16),
                pltpu.VMEM((HW // HEAD, 2 * JR, HEAD), BF16),
                pltpu.VMEM((JR, HW), BF16),
                pltpu.VMEM((2, 8, D), F32),
                pltpu.VMEM((2 * JR, HEAD), F32),
                pltpu.VMEM((2 * JR, HEAD), F32),
                pltpu.SemaphoreType.DMA((len(SEMS), 4)),
                pltpu.SemaphoreType.DMA((len(SEMS), 4)),
                pltpu.SemaphoreType.REGULAR((4,)),
                pltpu.SemaphoreType.DMA((WS,)),
                pltpu.SemaphoreType.DMA((2,)),
                pltpu.SemaphoreType.DMA,
                pltpu.SemaphoreType.DMA,
            ],
            compiler_params=pltpu.CompilerParams(collective_id=0, has_side_effects=True, vmem_limit_bytes=67043328),
            name="layer",
        )(x.reshape(NI, 2, 2, 4, C, D), x.reshape(NJ, JR, D), gain_a.reshape(-1, HEAD), gain_m.reshape(-1, HEAD), wq, wk, wv, wo, w_gate, w_up, w_down)
        return yb[NI:].reshape(x.shape)

    tokens, whole, columns, rows_of = P("dp", None, None), P(None), P(None, "tp"), P("tp", None)
    return jax.shard_map(
        step,
        mesh=mesh,
        in_specs=(tokens, whole, columns, columns, columns, rows_of, whole, columns, columns, rows_of),
        out_specs=tokens,
        check_vma=False,
    )
```

```python
import functools
import math

import jax
import jax.numpy as jnp
from jax import lax
from jax.experimental import pallas as pl
from jax.experimental.pallas import tpu as pltpu
from jax.sharding import PartitionSpec as P

HEAD = 128
THETA = 10000
F32, BF16 = jnp.float32, jnp.bfloat16

JR = 256
R = JR // 2
RH = R // 2
C = RH // 8
NJ = 8
NI = 2 * NJ
NT = 2 * NI
OS = 7
OT = 4
WS = 4
MP = 13
NP = 9
AT_MLP = 100
D, HW, FL = 8192, 512, 1536
CY = 4992
CZ = D - CY
KH, GK, PW = D // 2, 1024, 512
NS = 8
AT = {"sd": (0, 0), "s0": (0, 2), "s1": (0, 6), "s2": (1, 3), "s3": (2, 0), "s4": (2, 4), "s5": (3, 1), "s6": (3, 5), "s7": (4, 2), "s8": (4, 6), "s9": (5, 0)}
LAST = NT - 1 + AT["s9"][0]
LAST_CREDIT = NT - 1 + AT["s3"][0]

SEMS = ["D", "ZR", "gZR", "gD", "gR0"] + [f"YR{q}" for q in range(4)] + [f"gR{s}{j}" for s in "+-" for j in (1, 2, 3)] + [f"{g}{p}{s}{j}" for g in ("", "g") for p in "YZ" for s in "+-" for j in (1, 2, 3)]
SEM = {n: i for i, n in enumerate(SEMS)}


def _dot(a, b, ca=1, cb=0):
    return lax.dot_general(a, b, (((ca,), (cb,)), ((), ())), preferred_element_type=F32)


def kernel(x_ref, xj_ref, ga_ref, gm_ref, wq_ref, wk_ref, wv_ref, wo_ref, wg_ref, wu_ref, wd_ref, yb_ref,
           own, oth, drx, yrs, yrr, yls, ylr, zls, zlr, zrs, zrr, och, xch, hst, ablk, wsl, acc, hid, kst, vst, seen, gain, cos_ref, sin_ref,
           ssem, rsem, cred, wsem, asem, xsem, osem):
    t = lax.axis_index("tp")
    c, z, y = lax.rem(t, 2), lax.rem(lax.div(t, 2), 4), lax.div(t, 8)

    def at(y_, z_, c_):
        return (y_ * 4 + z_) * 2 + c_

    peer = {"c": at(y, z, 1 - c), "y": at(1 - y, z, c), "+": at(y, jnp.minimum(z + 1, 3), c), "-": at(y, jnp.maximum(z - 1, 0), c)}

    def signal(sem, to):
        pl.semaphore_signal(sem, inc=1, device_id={"tp": peer[to]}, device_id_type=pl.DeviceIdType.MESH)

    def each_peer(fn):
        fn("c")
        fn("y")
        pl.when(z > 0)(lambda: fn("-"))
        pl.when(z < 3)(lambda: fn("+"))

    barrier = pltpu.get_barrier_semaphore()
    each_peer(lambda p: signal(barrier, p))
    pl.when((z == 0) | (z == 3))(lambda: pl.semaphore_wait(barrier, 3))
    pl.when((z > 0) & (z < 3))(lambda: pl.semaphore_wait(barrier, 4))

    def rdma(name, par, src, dst, to):
        return pltpu.make_async_remote_copy(src_ref=src, dst_ref=dst, send_sem=ssem.at[SEM[name], par], recv_sem=rsem.at[SEM[name], par],
                                            device_id={"tp": peer[to]}, device_id_type=pl.DeviceIdType.MESH)

    NA = (NJ + 1) * 8
    NW = NA + NJ * 24

    def fetch(w):
        slot = lax.rem(w, WS)
        sem = wsem.at[slot]

        def go(src, lo, n):
            pltpu.make_async_copy(src, wsl.at[slot, pl.ds(lo, n), :], sem).start()

        @pl.when(w < NA)
        def _():
            j = lax.rem(w, 8)
            h = lax.rem(j, 2)
            for n, ref in enumerate((wq_ref, wk_ref, wv_ref)):
                pl.when(lax.div(j, 2) == n)(lambda ref=ref: go(ref.at[pl.ds(h * KH, KH), :], 0, KH))

            @pl.when(j >= 6)
            def _():
                for p in range(8):
                    go(wo_ref.at[:, pl.ds(h * KH + p * PW, PW)], p * HW, HW)

        @pl.when((w >= NA) & (w < NW))
        def _():
            u = lax.rem(w - NA, 24)
            for n, ref in enumerate((wg_ref, wu_ref)):
                @pl.when((u < 16) & (lax.rem(u, 2) == n))
                def _(ref=ref):
                    for p in range(3):
                        go(ref.at[pl.ds(lax.div(u, 2) * GK, GK), pl.ds(p * PW, PW)], p * GK, GK)

            @pl.when(u >= 16)
            def _():
                for p in range(2):
                    go(wd_ref.at[:, pl.ds((u - 16) * 2 * PW + p * PW, PW)], p * FL, FL)

    def tile_wait(w, rows):
        slot = lax.rem(w, WS)
        ref = wsl.at[slot, pl.ds(0, rows), :]
        pltpu.make_async_copy(ref, ref, wsem.at[slot]).wait()
        return slot

    def rows_start(job):
        slot = lax.rem(job, 2)

        def eight(q, _):
            item, u, v = lax.div(q, 16), lax.rem(lax.div(q, 4), 2), lax.rem(q, 4)

            half = lax.rem(lax.div(q, 8), 2)
            src = yb_ref.at[2 * (job - NJ) + item, lax.rem(c + half, 2), u, v]
            at_row = pl.multiple_of(half * R + item * RH + (u * 4 + v) * C, C)
            pltpu.make_async_copy(src, ablk.at[slot, pl.ds(at_row, C), :], asem.at[slot]).start()

        pl.when(job < NJ)(pltpu.make_async_copy(xj_ref.at[jnp.minimum(job, NJ - 1)], ablk.at[slot], asem.at[slot]).start)
        pl.when((job >= NJ) & (job < 2 * NJ))(lambda: lax.fori_loop(0, 32, eight, None))

    def rows_wait(job):
        slot = lax.rem(job, 2)
        pltpu.make_async_copy(ablk.at[slot], ablk.at[slot], asem.at[slot]).wait()

    def put(item, out, col):
        cols = pl.ds(pl.multiple_of(col, PW), PW)
        n = out.shape[0] // R
        for q in range(n):
            own[lax.rem(item + q, OS), :, :, :, cols] = out[q * RH : (q + 1) * RH].reshape(2, 4, C, PW)
            oth[lax.rem(item + q, OT), :, :, :, cols] = out[(n + q) * RH : (n + q + 1) * RH].reshape(2, 4, C, PW).astype(BF16)

    def attention_part(step, n, size):
        job = jnp.maximum(step - 1, 0)
        item = step if size == R else 2 * job
        at_row = step * R if size == R else 0
        mine = pl.ds(pl.multiple_of(at_row, R), size)
        ab = lax.rem(job, 2)
        half = lax.rem(job, 2)
        w = step * 8

        pl.when((n == 0) & (step != 1))(lambda: rows_wait(job))

        @pl.when((n == 0) & (step == 0))
        def _():
            for q in range(2, WS):
                fetch(q)

        @pl.when(n < size // R)
        def _():
            def norm(g, _):
                rows = pl.ds(pl.multiple_of(at_row + n * R + g * 32, 32), 32)
                total = jnp.zeros((32, HEAD), F32)
                for j in range(0, D, GK):
                    v = ablk[ab, rows, j : j + GK].astype(F32)
                    v = v * v
                    for q in range(0, GK, HEAD):
                        total += v[:, q : q + HEAD]
                scale = lax.rsqrt(jnp.sum(total, -1, keepdims=True) * (1 / D) + 1e-6)
                for j in range(0, D, GK):
                    v = ablk[ab, rows, j : j + GK].astype(F32) * scale
                    v = v.reshape(4, 8, GK) * gain[0, :, j : j + GK]
                    ablk[ab, rows, j : j + GK] = v.reshape(32, GK).astype(BF16)

            lax.fori_loop(0, R // 32, norm, None)

        @pl.when((n >= 2) & (n < 5))
        def _():
            tile = w + (n - 2) * 2
            slots = [tile_wait(tile + q, KH) for q in range(2)]
            cols = pl.ds(pl.multiple_of((n - 2) * PW, PW), PW)
            acc[0, mine, cols] = _dot(ablk[ab, mine, :KH], wsl[slots[0]]) + _dot(ablk[ab, mine, KH:], wsl[slots[1]])
            for q in range(2):
                fetch(tile + q + WS)

        @pl.when((n == 5) | (n == 6))
        def _():
            first = (n - 5) * 2
            col = pl.multiple_of(first * HEAD, 2 * HEAD)
            place = pl.ds(pl.multiple_of(half * JR + at_row, R), size)
            cos, sin = cos_ref[place, :], sin_ref[place, :]

            def column(at_col, i):
                return acc[0, mine, pl.ds(pl.multiple_of(at_col + col + i * HEAD, HEAD), HEAD)].astype(BF16)

            def turn(at_col, i):
                v = column(at_col, i).astype(F32)
                return (v * cos + pltpu.roll(v, HEAD // 2, 1) * sin).astype(BF16)

            qs = [turn(0, i) for i in range(2)]
            for i in range(2):
                kst[first + i, place, :] = turn(PW, i)
                vst[first + i, place, :] = column(2 * PW, i)

            def attend(seen_keys):
                for i in range(2):
                    s = _dot(qs[i], kst[first + i, :seen_keys, :], 1, 1) * HEAD**-0.5
                    token = lax.broadcasted_iota(jnp.int32, s.shape, 0) + (seen_keys - size)
                    s = jnp.where(token >= lax.broadcasted_iota(jnp.int32, s.shape, 1), s, -1e30)
                    p = jnp.exp(s - s.max(-1, keepdims=True))
                    p = (p * (1 / p.sum(-1, keepdims=True))).astype(BF16)
                    o = _dot(p, vst[first + i, :seen_keys, :]).astype(BF16)
                    for h in range(size // RH):
                        to_row = lax.rem(c + h, 2) * (size // 2) + (h // 2) * RH
                        seen[pl.ds(pl.multiple_of(to_row, RH), RH), pl.ds(pl.multiple_of(col + i * HEAD, HEAD), HEAD)] = o[h * RH : (h + 1) * RH]

            early = step == 0 if size == R else half == 0
            pl.when(early)(lambda: attend(size))
            pl.when(~early)(lambda: attend(2 * size))

        @pl.when(n >= 7)
        def _():
            tile = w + n - 1
            slot = tile_wait(tile, KH)
            for p in range(8):
                put(item, _dot(seen[:size], wsl[slot, p * HW : (p + 1) * HW, :]), (n - 7) * KH + p * PW)
            fetch(tile + WS)

    def mlp_part(job, u):
        ab = lax.rem(job, 2)
        w = NA + (job - NJ) * 24 + 2 * jnp.where(u < 8, u, u - 1)

        @pl.when(u == 0)
        def _():
            rows_wait(job)
            acc[...] = jnp.zeros((2, JR, FL), F32)

        @pl.when(u < 8)
        def _():
            slots = [tile_wait(w + q, 3 * GK) for q in range(2)]
            lhs = ablk[ab, :, pl.ds(pl.multiple_of(u * GK, GK), GK)]
            for q in range(2):
                for p in range(3):
                    acc[q, :, p * PW : (p + 1) * PW] += _dot(lhs, wsl[slots[q], p * GK : (p + 1) * GK, :])
            for q in range(2):
                fetch(w + q + WS)

        @pl.when(u == 8)
        def _():
            def rows(g, _):
                r = pl.ds(pl.multiple_of(g * 16, 16), 16)
                gate = acc[0, r, :]
                hid[r, :] = (gate * (1 / (1 + jnp.exp(-gate))) * acc[1, r, :]).astype(BF16)

            lax.fori_loop(0, JR // 16, rows, None)

        @pl.when(u > 8)
        def _():
            slots = [tile_wait(w + q, 3 * GK) for q in range(2)]
            for q in range(2):
                for p in range(2):
                    put(2 * job, _dot(hid[...], wsl[slots[q], p * FL : (p + 1) * FL, :]), ((u - 9) * 2 + q) * 2 * PW + p * PW)
            for q in range(2):
                fetch(w + q + WS)

    def rs_send(s, j):
        return ((z < 3) & (j > z), 4 + z - j) if s == "+" else ((z > 0) & (j >= 4 - z), j + z - 4)

    def rs_recv(s, j):
        return (z >= 1) & (j >= z) if s == "+" else (z <= 2) & (j >= 3 - z)

    def first(s):
        return z == 0 if s == "+" else z == 3

    def ag_send(s, j):
        return ((z < 3) & (j <= z + 1), z - (j - 1)) if s == "+" else ((z > 0) & (j <= 4 - z), z + (j - 1))

    def ag_recv(s, j):
        return ((z >= 1) & (j <= z), z - j) if s == "+" else ((z <= 2) & (j <= 3 - z), z + j)

    YC, ZC = pl.ds(0, CY), pl.ds(CY, CZ)
    S = {"+": 0, "-": 1}

    def core(i, par):
        return rdma("D", par, oth.at[lax.rem(i, OT)], drx.at[par], "c")

    def sd(i, par):
        pl.when((i < 2) | (par == 0))(core(i, par).start)
        pl.when((i >= 2) & (par == 0))(core(i + 1, 1).start)

    def y_line(i, par, j):
        for s in "+-":
            yes, k = rs_send(s, j)

            @pl.when(yes & first(s))
            def _():
                yls[S[s], j - 1] = own[lax.rem(i, OS), y, k, :, YC].astype(BF16)

            if j > 1:
                @pl.when(yes & ~first(s))
                def _():
                    yls[S[s], j - 1] = (own[lax.rem(i, OS), y, k, :, YC] + ylr[par, S[s], j - 2].astype(F32)).astype(BF16)

            pl.when(yes)(rdma(f"Y{s}{j}", par, yls.at[S[s], j - 1], ylr.at[par, S[s], j - 1], s).start)

    def z_line(i, par, j):
        for s in "+-":
            yes, k = rs_send(s, j)

            @pl.when(yes & first(s))
            def _():
                for h in range(2):
                    zls[S[s], j - 1, h] = own[lax.rem(i, OS), h, k, :, ZC].astype(BF16)

            if j > 1:
                @pl.when(yes & ~first(s))
                def _():
                    for h in range(2):
                        zls[S[s], j - 1, h] = (own[lax.rem(i, OS), h, k, :, ZC] + zlr[par, S[s], j - 2, h].astype(F32)).astype(BF16)

            pl.when(yes)(rdma(f"Z{s}{j}", par, zls.at[S[s], j - 1], zlr.at[par, S[s], j - 1], s).start)

    def line_wait(part, par, j):
        sb, rb = (yls, ylr) if part == "Y" else (zls, zlr)
        for s in "+-":
            cp = rdma(f"{part}{s}{j}", par, sb.at[S[s], j - 1], rb.at[par, S[s], j - 1], s)
            pl.when(rs_send(s, j)[0])(cp.wait_send)
            pl.when(rs_recv(s, j))(cp.wait_recv)

    def piece(q):
        return (jnp.where(z < 2, 3, 0), jnp.where(z < 2, 2, 1), jnp.where(z < 2, 1 - z, 5 - z), z)[q]

    def rung(i, par, q):
        four = lax.rem(i, 4)
        return rdma(f"YR{q}", four, yrs.at[par, q], yrr.at[four, q], "y")

    def rung_add(i, par, q):
        rung(i, par, q).wait_recv()
        own[lax.rem(i, OS), y, piece(q), :, YC] += yrr[lax.rem(i, 4), q].astype(F32)

    def s0(i, par):
        core(i, par).wait()
        slot = lax.rem(i, OS)

        def add(k, _):
            a, b = lax.div(k, 4), lax.rem(k, 4)
            own[slot, a, b] += drx[par, a, b].astype(F32)

        lax.fori_loop(0, 8, add, None)

        for q in range(4):
            yrs[par, q] = own[slot, 1 - y, piece(q), :, YC].astype(BF16)
            rung(i, par, q).start()
            if q == 0:
                z_line(i, par, 1)

    def s1(i, par):
        rung_add(i, par, 0)
        y_line(i, par, 1)
        line_wait("Z", par, 1)
        z_line(i, par, 2)

    def s2(i, par):
        for q in range(4):
            rung(i, par, q).wait_send()
        rung_add(i, par, 1)
        line_wait("Y", par, 1)
        y_line(i, par, 2)
        line_wait("Z", par, 2)
        z_line(i, par, 3)

    def x_copy(i):
        return pltpu.make_async_copy(x_ref.at[i, c, y, z], xch, xsem)

    def s3(i, par):
        pl.when(i < NI)(lambda: x_copy(i).start())
        rung_add(i, par, 2)
        line_wait("Y", par, 2)
        y_line(i, par, 3)
        line_wait("Z", par, 3)
        slot = lax.rem(i, OS)
        for s in "+-":
            @pl.when(rs_recv(s, 3))
            def _():
                for h in range(2):
                    own[slot, h, z, :, ZC] += zlr[par, S[s], 2, h].astype(F32)
        zrs[...] = own[slot, 1 - y, z, :, ZC].astype(BF16)
        rdma("ZR", par, zrs, zrr.at[par], "y").start()

    def och_copy(i):
        return pltpu.make_async_copy(och, yb_ref.at[i, c, y, z], osem)

    def ag_first(i, par):
        cps = [(ag_send(s, 1)[0], ag_recv(s, 1)[0], rdma(f"gY{s}1", lax.rem(i, 4), och.at[:, YC], yb_ref.at[i, c, y, z, :, YC], s)) for s in "+-"]
        return cps, rdma("gZR", lax.rem(i, 4), och.at[:, ZC], yb_ref.at[i, c, y, z, :, ZC], "y")

    def s4(i, par):
        slot = lax.rem(i, OS)
        rung_add(i, par, 3)
        line_wait("Y", par, 3)
        for s in "+-":
            @pl.when(rs_recv(s, 3))
            def _():
                own[slot, y, z, :, YC] += ylr[par, S[s], 2].astype(F32)
        rdma("ZR", par, zrs, zrr.at[par], "y").wait()
        own[slot, y, z, :, ZC] += zrr[par].astype(F32)

        @pl.when(i < NI)
        def _():
            x_copy(i).wait()
            h = (xch[...].astype(F32) + own[slot, y, z]).astype(BF16)
            hst[i] = h
            v = h.astype(F32)
            scale = lax.rsqrt(jnp.mean(v * v, -1, keepdims=True) + 1e-6)
            och[...] = (v * scale * gain[1]).astype(BF16)

        @pl.when(i >= NI)
        def _():
            och[...] = (hst[i - NI].astype(F32) + own[slot, y, z]).astype(BF16)

        och_copy(i).start()
        lines, rung = ag_first(i, par)
        for yes, _, cp in lines:
            pl.when(yes)(cp.start)
        g_rung(i, "0").start()
        rung.start()

    def ag_y(i, par, j):
        return [(*ag_send(s, j), *ag_recv(s, j), s) for s in "+-"]

    def g_src(part, i, k):
        return yb_ref.at[i, c, y, k, :, YC] if part == "Y" else yb_ref.at[i, c, :, k, :, ZC]

    def g_line(part, i, par, j):
        for s in "+-":
            yes, k = ag_send(s, j)

            @pl.when(yes)
            def _():
                rdma(f"g{part}{s}{j}", lax.rem(i, 4), g_src(part, i, k), g_src(part, i, k), s).start()

    def g_wait(part, i, par, j):
        for s in "+-":
            yes, k = ag_send(s, j)
            got, _ = ag_recv(s, j)
            ref = g_src(part, i, 0)
            cp = rdma(f"g{part}{s}{j}", lax.rem(i, 4), ref, ref, s)
            pl.when(yes)(cp.wait_send)
            pl.when(got)(cp.wait_recv)

    def s5(i, par):
        och_copy(i).wait()
        lines, rung = ag_first(i, par)
        for yes, got, cp in lines:
            pl.when(yes)(cp.wait_send)
            pl.when(got)(cp.wait_recv)
        g_rung(i, "0").wait_send()
        g_line("Y", i, par, 2)
        g_rungs(i, 1)
        rung.wait()
        g_line("Z", i, par, 1)

    def s6(i, par):
        g_wait("Y", i, par, 2)
        g_line("Y", i, par, 3)
        g_rungs(i, 2)
        g_wait("Z", i, par, 1)
        g_line("Z", i, par, 2)

    def g_rung(i, name, k=0):
        ref = yb_ref.at[i, c, y, k, :, YC]
        return rdma("gR" + name, lax.rem(i, 4), och.at[:, YC] if name == "0" else ref, yb_ref.at[i, c, y, z, :, YC] if name == "0" else ref, "y")

    def g_rungs(i, j):
        for s in "+-":
            got, k = ag_recv(s, j)
            pl.when(got)(lambda: g_rung(i, f"{s}{j}", k).start())

    def g_core(i, par):
        ref = yb_ref.at[i, c]
        return rdma("gD", lax.rem(i, 4), ref, ref, "c")

    def s7(i, par):
        g_wait("Y", i, par, 3)
        g_rungs(i, 3)
        g_wait("Z", i, par, 2)
        g_line("Z", i, par, 3)

    def s8(i, par):
        g_wait("Z", i, par, 3)
        g_rung(i, "0").wait_recv()
        for j in (1, 2, 3):
            for s in "+-":
                pl.when(ag_recv(s, j)[0])(lambda: g_rung(i, f"{s}{j}").wait())
        g_core(i, par).start()

    def s9(i, par):
        g_core(i, par).wait()

    actions = [("sd", sd), ("s0", s0), ("s1", s1), ("s2", s2), ("s3", s3), ("s4", s4), ("s5", s5), ("s6", s6), ("s7", s7), ("s8", s8), ("s9", s9)]
    order = sorted(actions, key=lambda a: -AT[a[0]][0])

    CR = {"c": 0, "y": 1, "-": 2, "+": 3}
    BACK = {"c": 0, "y": 1, "-": 3, "+": 2}

    rows_start(0)
    fetch(0)
    fetch(1)
    for n, ref in enumerate((ga_ref, gm_ref)):
        for q in range(D // HEAD):
            gain[n, :, q * HEAD : (q + 1) * HEAD] = jnp.broadcast_to(ref[q : q + 1, :].astype(F32), (8, HEAD))

    def turns(g, _):
        shape = (64, HEAD)
        lane = lax.broadcasted_iota(jnp.int32, shape, 1)
        place = (lax.broadcasted_iota(jnp.int32, shape, 0) + g * 64).astype(F32)
        angle = place * jnp.exp(lax.rem(lane, HEAD // 2).astype(F32) * (-math.log(THETA) / (HEAD // 2)))
        rows = pl.ds(pl.multiple_of(g * 64, 64), 64)
        cos_ref[rows, :] = jnp.cos(angle)
        sin_ref[rows, :] = jnp.where(lane < HEAD // 2, -1.0, 1.0) * jnp.sin(angle)

    lax.fori_loop(0, 2 * JR // 64, turns, None)

    def parts_by(m):
        n = jnp.maximum(m - 1, 0)

        def over(start, a, b, most):
            return jnp.minimum(lax.div(jnp.maximum(n - start, 0) * a, b), most)

        return jnp.minimum(m, 1) * NP + over(0, 9, 7, NP) + over(7, 1, 1, NP) + over(16, 9, 14, (NJ - 2) * NP) + over(AT_MLP, 16, 21, MP * NJ)

    def compute(n, _):
        ends = (NJ + 1) * NP

        @pl.when(n < ends)
        def _():
            step, part = lax.div(n, NP), lax.rem(n, NP)
            pl.when((part == 2) & (step >= 1))(lambda: rows_start(step))
            pl.when(step < 2)(lambda: attention_part(step, part, R))
            pl.when(step >= 2)(lambda: attention_part(step, part, JR))

        @pl.when(n >= ends)
        def _():
            job, part = NJ + lax.div(n - ends, MP), lax.rem(n - ends, MP)
            pl.when(part == 4)(lambda: rows_start(job + 1))
            mlp_part(job, part)

    def body(m, _):
        k, n = lax.div(m + NS - 1, NS) - 1, lax.rem(m + NS - 1, NS)
        pl.when((n == 0) & (k >= 1) & (k <= LAST_CREDIT))(lambda: each_peer(lambda p: pl.semaphore_wait(cred.at[CR[p]], 1)))
        for name, fn in order:
            d, pos = AT[name]
            i = k - d
            pl.when((n == pos) & (i >= 0) & (i < NT))(lambda fn=fn, i=i: fn(i, lax.rem(i, 2)))
        lax.fori_loop(parts_by(m), parts_by(m + 1), compute, None)
        pl.when((n == 5) & (k >= 0) & (k < LAST_CREDIT))(lambda: each_peer(lambda p: signal(cred.at[BACK[p]], p)))

    lax.fori_loop(0, LAST * NS + AT["s9"][1] + 2, body, None)


def solution(mesh):
    def step(x, gain_a, wq, wk, wv, wo, gain_m, w_gate, w_up, w_down):
        batch, rows, d = x.shape
        hbm, vmem = pl.BlockSpec(memory_space=pl.ANY), pl.BlockSpec(memory_space=pltpu.VMEM)
        yb = pl.pallas_call(
            kernel,
            out_shape=jax.ShapeDtypeStruct((NT, 2, 2, 4, C, D), BF16),
            in_specs=[hbm, hbm, vmem, vmem] + [hbm] * 7,
            out_specs=hbm,
            scratch_shapes=[
                pltpu.VMEM((OS, 2, 4, C, D), F32),
                pltpu.VMEM((OT, 2, 4, C, D), BF16),
                pltpu.VMEM((2, 2, 4, C, D), BF16),
                pltpu.VMEM((2, 4, C, CY), BF16),
                pltpu.VMEM((4, 4, C, CY), BF16),
                pltpu.VMEM((2, 3, C, CY), BF16),
                pltpu.VMEM((2, 2, 3, C, CY), BF16),
                pltpu.VMEM((2, 3, 2, C, CZ), BF16),
                pltpu.VMEM((2, 2, 3, 2, C, CZ), BF16),
                pltpu.VMEM((C, CZ), BF16),
                pltpu.VMEM((2, C, CZ), BF16),
                pltpu.VMEM((C, D), BF16),
                pltpu.VMEM((C, D), BF16),
                pltpu.VMEM((NI, C, D), BF16),
                pltpu.VMEM((2, JR, D), BF16),
                pltpu.VMEM((WS, KH, PW), BF16),
                pltpu.VMEM((2, JR, FL), F32),
                pltpu.VMEM((JR, FL), BF16),
                pltpu.VMEM((HW // HEAD, 2 * JR, HEAD), BF16),
                pltpu.VMEM((HW // HEAD, 2 * JR, HEAD), BF16),
                pltpu.VMEM((JR, HW), BF16),
                pltpu.VMEM((2, 8, D), F32),
                pltpu.VMEM((2 * JR, HEAD), F32),
                pltpu.VMEM((2 * JR, HEAD), F32),
                pltpu.SemaphoreType.DMA((len(SEMS), 4)),
                pltpu.SemaphoreType.DMA((len(SEMS), 4)),
                pltpu.SemaphoreType.REGULAR((4,)),
                pltpu.SemaphoreType.DMA((WS,)),
                pltpu.SemaphoreType.DMA((2,)),
                pltpu.SemaphoreType.DMA,
                pltpu.SemaphoreType.DMA,
            ],
            compiler_params=pltpu.CompilerParams(collective_id=0, has_side_effects=True, vmem_limit_bytes=67043328),
            name="layer",
        )(x.reshape(NI, 2, 2, 4, C, D), x.reshape(NJ, JR, D), gain_a.reshape(-1, HEAD), gain_m.reshape(-1, HEAD), wq, wk, wv, wo, w_gate, w_up, w_down)
        return yb[NI:].reshape(x.shape)

    tokens, whole, columns, rows_of = P("dp", None, None), P(None), P(None, "tp"), P("tp", None)
    return jax.shard_map(
        step,
        mesh=mesh,
        in_specs=(tokens, whole, columns, columns, columns, rows_of, whole, columns, columns, rows_of),
        out_specs=tokens,
        check_vma=False,
    )
```

```python
import functools
import math

import jax
import jax.numpy as jnp
from jax import lax
from jax.experimental import pallas as pl
from jax.experimental.pallas import tpu as pltpu
from jax.sharding import PartitionSpec as P

HEAD = 128
THETA = 10000
F32, BF16 = jnp.float32, jnp.bfloat16

JR = 256
R = JR // 2
RH = R // 2
C = RH // 8
NJ = 8
NI = 2 * NJ
NT = 2 * NI
OS = 7
OT = 4
WS = 4
MP = 13
NP = 9
AT_MLP = 100
D, HW, FL = 8192, 512, 1536
CY = 4992
CZ = D - CY
KH, GK, PW = D // 2, 1024, 512
NS = 8
AT = {"sd": (0, 0), "s0": (0, 2), "s1": (0, 6), "s2": (1, 3), "s3": (2, 0), "s4": (2, 4), "s5": (3, 1), "s6": (3, 5), "s7": (4, 2), "s8": (4, 6), "s9": (5, 0)}
LAST = NT - 1 + AT["s9"][0]
LAST_CREDIT = NT - 1 + AT["s3"][0]

SEMS = ["D", "ZR", "gZR", "gD", "gR0"] + [f"YR{q}" for q in range(4)] + [f"gR{s}{j}" for s in "+-" for j in (1, 2, 3)] + [f"{g}{p}{s}{j}" for g in ("", "g") for p in "YZ" for s in "+-" for j in (1, 2, 3)]
SEM = {n: i for i, n in enumerate(SEMS)}


def _dot(a, b, ca=1, cb=0):
    return lax.dot_general(a, b, (((ca,), (cb,)), ((), ())), preferred_element_type=F32)


def kernel(x_ref, xj_ref, ga_ref, gm_ref, wq_ref, wk_ref, wv_ref, wo_ref, wg_ref, wu_ref, wd_ref, yb_ref,
           own, oth, drx, yrs, yrr, yls, ylr, zls, zlr, zrs, zrr, och, xch, hst, ablk, wsl, acc, hid, kst, vst, seen, gain, cos_ref, sin_ref,
           ssem, rsem, cred, wsem, asem, xsem, osem):
    t = lax.axis_index("tp")
    c, z, y = lax.rem(t, 2), lax.rem(lax.div(t, 2), 4), lax.div(t, 8)

    def at(y_, z_, c_):
        return (y_ * 4 + z_) * 2 + c_

    peer = {"c": at(y, z, 1 - c), "y": at(1 - y, z, c), "+": at(y, jnp.minimum(z + 1, 3), c), "-": at(y, jnp.maximum(z - 1, 0), c)}

    def signal(sem, to):
        pl.semaphore_signal(sem, inc=1, device_id={"tp": peer[to]}, device_id_type=pl.DeviceIdType.MESH)

    def each_peer(fn):
        fn("c")
        fn("y")
        pl.when(z > 0)(lambda: fn("-"))
        pl.when(z < 3)(lambda: fn("+"))

    barrier = pltpu.get_barrier_semaphore()
    each_peer(lambda p: signal(barrier, p))
    pl.when((z == 0) | (z == 3))(lambda: pl.semaphore_wait(barrier, 3))
    pl.when((z > 0) & (z < 3))(lambda: pl.semaphore_wait(barrier, 4))

    def rdma(name, par, src, dst, to):
        return pltpu.make_async_remote_copy(src_ref=src, dst_ref=dst, send_sem=ssem.at[SEM[name], par], recv_sem=rsem.at[SEM[name], par],
                                            device_id={"tp": peer[to]}, device_id_type=pl.DeviceIdType.MESH)

    NA = (NJ + 1) * 8
    NW = NA + NJ * 24

    def fetch(w):
        slot = lax.rem(w, WS)
        sem = wsem.at[slot]

        def go(src, lo, n):
            pltpu.make_async_copy(src, wsl.at[slot, pl.ds(lo, n), :], sem).start()

        @pl.when(w < NA)
        def _():
            j = lax.rem(w, 8)
            h = lax.rem(j, 2)
            for n, ref in enumerate((wq_ref, wk_ref, wv_ref)):
                pl.when(lax.div(j, 2) == n)(lambda ref=ref: go(ref.at[pl.ds(h * KH, KH), :], 0, KH))

            @pl.when(j >= 6)
            def _():
                for p in range(8):
                    go(wo_ref.at[:, pl.ds(h * KH + p * PW, PW)], p * HW, HW)

        @pl.when((w >= NA) & (w < NW))
        def _():
            u = lax.rem(w - NA, 24)
            for n, ref in enumerate((wg_ref, wu_ref)):
                @pl.when((u < 16) & (lax.rem(u, 2) == n))
                def _(ref=ref):
                    for p in range(3):
                        go(ref.at[pl.ds(lax.div(u, 2) * GK, GK), pl.ds(p * PW, PW)], p * GK, GK)

            @pl.when(u >= 16)
            def _():
                for p in range(2):
                    go(wd_ref.at[:, pl.ds((u - 16) * 2 * PW + p * PW, PW)], p * FL, FL)

    def tile_wait(w, rows):
        slot = lax.rem(w, WS)
        ref = wsl.at[slot, pl.ds(0, rows), :]
        pltpu.make_async_copy(ref, ref, wsem.at[slot]).wait()
        return slot

    def rows_start(job):
        slot = lax.rem(job, 2)

        def eight(q, _):
            item, u, v = lax.div(q, 16), lax.rem(lax.div(q, 4), 2), lax.rem(q, 4)

            half = lax.rem(lax.div(q, 8), 2)
            src = yb_ref.at[2 * (job - NJ) + item, lax.rem(c + half, 2), u, v]
            at_row = pl.multiple_of(half * R + item * RH + (u * 4 + v) * C, C)
            pltpu.make_async_copy(src, ablk.at[slot, pl.ds(at_row, C), :], asem.at[slot]).start()

        pl.when(job < NJ)(pltpu.make_async_copy(xj_ref.at[jnp.minimum(job, NJ - 1)], ablk.at[slot], asem.at[slot]).start)
        pl.when((job >= NJ) & (job < 2 * NJ))(lambda: lax.fori_loop(0, 32, eight, None))

    def rows_wait(job):
        slot = lax.rem(job, 2)
        pltpu.make_async_copy(ablk.at[slot], ablk.at[slot], asem.at[slot]).wait()

    def put(item, out, col):
        cols = pl.ds(pl.multiple_of(col, PW), PW)
        n = out.shape[0] // R
        for q in range(n):
            own[lax.rem(item + q, OS), :, :, :, cols] = out[q * RH : (q + 1) * RH].reshape(2, 4, C, PW)
            oth[lax.rem(item + q, OT), :, :, :, cols] = out[(n + q) * RH : (n + q + 1) * RH].reshape(2, 4, C, PW).astype(BF16)

    def attention_part(step, n, size):
        job = jnp.maximum(step - 1, 0)
        item = step if size == R else 2 * job
        at_row = step * R if size == R else 0
        mine = pl.ds(pl.multiple_of(at_row, R), size)
        ab = lax.rem(job, 2)
        half = lax.rem(job, 2)
        w = step * 8

        pl.when((n == 0) & (step != 1))(lambda: rows_wait(job))

        @pl.when((n == 0) & (step == 0))
        def _():
            for q in range(2, WS):
                fetch(q)

        @pl.when(n < size // R)
        def _():
            def norm(g, _):
                rows = pl.ds(pl.multiple_of(at_row + n * R + g * 32, 32), 32)
                total = jnp.zeros((32, HEAD), F32)
                for j in range(0, D, GK):
                    v = ablk[ab, rows, j : j + GK].astype(F32)
                    v = v * v
                    for q in range(0, GK, HEAD):
                        total += v[:, q : q + HEAD]
                scale = lax.rsqrt(jnp.sum(total, -1, keepdims=True) * (1 / D) + 1e-6)
                for j in range(0, D, GK):
                    v = ablk[ab, rows, j : j + GK].astype(F32) * scale
                    v = v.reshape(4, 8, GK) * gain[0, :, j : j + GK]
                    ablk[ab, rows, j : j + GK] = v.reshape(32, GK).astype(BF16)

            lax.fori_loop(0, R // 32, norm, None)

        @pl.when((n >= 2) & (n < 5))
        def _():
            tile = w + (n - 2) * 2
            slots = [tile_wait(tile + q, KH) for q in range(2)]
            cols = pl.ds(pl.multiple_of((n - 2) * PW, PW), PW)
            acc[0, mine, cols] = _dot(ablk[ab, mine, :KH], wsl[slots[0]]) + _dot(ablk[ab, mine, KH:], wsl[slots[1]])
            for q in range(2):
                fetch(tile + q + WS)

        @pl.when((n == 5) | (n == 6))
        def _():
            first = (n - 5) * 2
            col = pl.multiple_of(first * HEAD, 2 * HEAD)
            place = pl.ds(pl.multiple_of(half * JR + at_row, R), size)
            cos, sin = cos_ref[place, :], sin_ref[place, :]

            def column(at_col, i):
                return acc[0, mine, pl.ds(pl.multiple_of(at_col + col + i * HEAD, HEAD), HEAD)].astype(BF16)

            def turn(at_col, i):
                v = column(at_col, i).astype(F32)
                return (v * cos + pltpu.roll(v, HEAD // 2, 1) * sin).astype(BF16)

            qs = [turn(0, i) for i in range(2)]
            for i in range(2):
                kst[first + i, place, :] = turn(PW, i)
                vst[first + i, place, :] = column(2 * PW, i)

            def attend(seen_keys):
                for i in range(2):
                    s = _dot(qs[i], kst[first + i, :seen_keys, :], 1, 1) * HEAD**-0.5
                    token = lax.broadcasted_iota(jnp.int32, s.shape, 0) + (seen_keys - size)
                    s = jnp.where(token >= lax.broadcasted_iota(jnp.int32, s.shape, 1), s, -jnp.inf)
                    p = jnp.exp(s - s.max(-1, keepdims=True))
                    p = (p * (1 / p.sum(-1, keepdims=True))).astype(BF16)
                    o = _dot(p, vst[first + i, :seen_keys, :]).astype(BF16)
                    for h in range(size // RH):
                        to_row = lax.rem(c + h, 2) * (size // 2) + (h // 2) * RH
                        seen[pl.ds(pl.multiple_of(to_row, RH), RH), pl.ds(pl.multiple_of(col + i * HEAD, HEAD), HEAD)] = o[h * RH : (h + 1) * RH]

            early = step == 0 if size == R else half == 0
            pl.when(early)(lambda: attend(size))
            pl.when(~early)(lambda: attend(2 * size))

        @pl.when(n >= 7)
        def _():
            tile = w + n - 1
            slot = tile_wait(tile, KH)
            for p in range(8):
                put(item, _dot(seen[:size], wsl[slot, p * HW : (p + 1) * HW, :]), (n - 7) * KH + p * PW)
            fetch(tile + WS)

    def mlp_part(job, u):
        ab = lax.rem(job, 2)
        w = NA + (job - NJ) * 24 + 2 * jnp.where(u < 8, u, u - 1)

        @pl.when(u == 0)
        def _():
            rows_wait(job)
            acc[...] = jnp.zeros((2, JR, FL), F32)

        @pl.when(u < 8)
        def _():
            slots = [tile_wait(w + q, 3 * GK) for q in range(2)]
            lhs = ablk[ab, :, pl.ds(pl.multiple_of(u * GK, GK), GK)]
            for q in range(2):
                for p in range(3):
                    acc[q, :, p * PW : (p + 1) * PW] += _dot(lhs, wsl[slots[q], p * GK : (p + 1) * GK, :])
            for q in range(2):
                fetch(w + q + WS)

        @pl.when(u == 8)
        def _():
            def rows(g, _):
                r = pl.ds(pl.multiple_of(g * 16, 16), 16)
                gate = acc[0, r, :]
                hid[r, :] = (gate * (1 / (1 + jnp.exp(-gate))) * acc[1, r, :]).astype(BF16)

            lax.fori_loop(0, JR // 16, rows, None)

        @pl.when(u > 8)
        def _():
            slots = [tile_wait(w + q, 3 * GK) for q in range(2)]
            for q in range(2):
                for p in range(2):
                    put(2 * job, _dot(hid[...], wsl[slots[q], p * FL : (p + 1) * FL, :]), ((u - 9) * 2 + q) * 2 * PW + p * PW)
            for q in range(2):
                fetch(w + q + WS)

    def rs_send(s, j):
        return ((z < 3) & (j > z), 4 + z - j) if s == "+" else ((z > 0) & (j >= 4 - z), j + z - 4)

    def rs_recv(s, j):
        return (z >= 1) & (j >= z) if s == "+" else (z <= 2) & (j >= 3 - z)

    def first(s):
        return z == 0 if s == "+" else z == 3

    def ag_send(s, j):
        return ((z < 3) & (j <= z + 1), z - (j - 1)) if s == "+" else ((z > 0) & (j <= 4 - z), z + (j - 1))

    def ag_recv(s, j):
        return ((z >= 1) & (j <= z), z - j) if s == "+" else ((z <= 2) & (j <= 3 - z), z + j)

    YC, ZC = pl.ds(0, CY), pl.ds(CY, CZ)
    S = {"+": 0, "-": 1}

    def core(i, par):
        return rdma("D", par, oth.at[lax.rem(i, OT)], drx.at[par], "c")

    def sd(i, par):
        pl.when((i < 2) | (par == 0))(core(i, par).start)
        pl.when((i >= 2) & (par == 0))(core(i + 1, 1).start)

    def y_line(i, par, j):
        for s in "+-":
            yes, k = rs_send(s, j)

            @pl.when(yes & first(s))
            def _():
                yls[S[s], j - 1] = own[lax.rem(i, OS), y, k, :, YC].astype(BF16)

            if j > 1:
                @pl.when(yes & ~first(s))
                def _():
                    yls[S[s], j - 1] = (own[lax.rem(i, OS), y, k, :, YC] + ylr[par, S[s], j - 2].astype(F32)).astype(BF16)

            pl.when(yes)(rdma(f"Y{s}{j}", par, yls.at[S[s], j - 1], ylr.at[par, S[s], j - 1], s).start)

    def z_line(i, par, j):
        for s in "+-":
            yes, k = rs_send(s, j)

            @pl.when(yes & first(s))
            def _():
                for h in range(2):
                    zls[S[s], j - 1, h] = own[lax.rem(i, OS), h, k, :, ZC].astype(BF16)

            if j > 1:
                @pl.when(yes & ~first(s))
                def _():
                    for h in range(2):
                        zls[S[s], j - 1, h] = (own[lax.rem(i, OS), h, k, :, ZC] + zlr[par, S[s], j - 2, h].astype(F32)).astype(BF16)

            pl.when(yes)(rdma(f"Z{s}{j}", par, zls.at[S[s], j - 1], zlr.at[par, S[s], j - 1], s).start)

    def line_wait(part, par, j):
        sb, rb = (yls, ylr) if part == "Y" else (zls, zlr)
        for s in "+-":
            cp = rdma(f"{part}{s}{j}", par, sb.at[S[s], j - 1], rb.at[par, S[s], j - 1], s)
            pl.when(rs_send(s, j)[0])(cp.wait_send)
            pl.when(rs_recv(s, j))(cp.wait_recv)

    def piece(q):
        return (jnp.where(z < 2, 3, 0), jnp.where(z < 2, 2, 1), jnp.where(z < 2, 1 - z, 5 - z), z)[q]

    def rung(i, par, q):
        four = lax.rem(i, 4)
        return rdma(f"YR{q}", four, yrs.at[par, q], yrr.at[four, q], "y")

    def rung_add(i, par, q):
        rung(i, par, q).wait_recv()
        own[lax.rem(i, OS), y, piece(q), :, YC] += yrr[lax.rem(i, 4), q].astype(F32)

    def s0(i, par):
        core(i, par).wait()
        slot = lax.rem(i, OS)

        def add(k, _):
            a, b = lax.div(k, 4), lax.rem(k, 4)
            own[slot, a, b] += drx[par, a, b].astype(F32)

        lax.fori_loop(0, 8, add, None)

        for q in range(4):
            yrs[par, q] = own[slot, 1 - y, piece(q), :, YC].astype(BF16)
            rung(i, par, q).start()
            if q == 0:
                z_line(i, par, 1)

    def s1(i, par):
        rung_add(i, par, 0)
        y_line(i, par, 1)
        line_wait("Z", par, 1)
        z_line(i, par, 2)

    def s2(i, par):
        for q in range(4):
            rung(i, par, q).wait_send()
        rung_add(i, par, 1)
        line_wait("Y", par, 1)
        y_line(i, par, 2)
        line_wait("Z", par, 2)
        z_line(i, par, 3)

    def x_copy(i):
        return pltpu.make_async_copy(x_ref.at[i, c, y, z], xch, xsem)

    def s3(i, par):
        pl.when(i < NI)(lambda: x_copy(i).start())
        rung_add(i, par, 2)
        line_wait("Y", par, 2)
        y_line(i, par, 3)
        line_wait("Z", par, 3)
        slot = lax.rem(i, OS)
        for s in "+-":
            @pl.when(rs_recv(s, 3))
            def _():
                for h in range(2):
                    own[slot, h, z, :, ZC] += zlr[par, S[s], 2, h].astype(F32)
        zrs[...] = own[slot, 1 - y, z, :, ZC].astype(BF16)
        rdma("ZR", par, zrs, zrr.at[par], "y").start()

    def och_copy(i):
        return pltpu.make_async_copy(och, yb_ref.at[i, c, y, z], osem)

    def ag_first(i, par):
        cps = [(ag_send(s, 1)[0], ag_recv(s, 1)[0], rdma(f"gY{s}1", lax.rem(i, 4), och.at[:, YC], yb_ref.at[i, c, y, z, :, YC], s)) for s in "+-"]
        return cps, rdma("gZR", lax.rem(i, 4), och.at[:, ZC], yb_ref.at[i, c, y, z, :, ZC], "y")

    def s4(i, par):
        slot = lax.rem(i, OS)
        rung_add(i, par, 3)
        line_wait("Y", par, 3)
        for s in "+-":
            @pl.when(rs_recv(s, 3))
            def _():
                own[slot, y, z, :, YC] += ylr[par, S[s], 2].astype(F32)
        rdma("ZR", par, zrs, zrr.at[par], "y").wait()
        own[slot, y, z, :, ZC] += zrr[par].astype(F32)

        @pl.when(i < NI)
        def _():
            x_copy(i).wait()
            h = (xch[...].astype(F32) + own[slot, y, z]).astype(BF16)
            hst[i] = h
            v = h.astype(F32)
            scale = lax.rsqrt(jnp.mean(v * v, -1, keepdims=True) + 1e-6)
            och[...] = (v * scale * gain[1]).astype(BF16)

        @pl.when(i >= NI)
        def _():
            och[...] = (hst[i - NI].astype(F32) + own[slot, y, z]).astype(BF16)

        och_copy(i).start()
        lines, rung = ag_first(i, par)
        for yes, _, cp in lines:
            pl.when(yes)(cp.start)
        g_rung(i, "0").start()
        rung.start()

    def ag_y(i, par, j):
        return [(*ag_send(s, j), *ag_recv(s, j), s) for s in "+-"]

    def g_src(part, i, k):
        return yb_ref.at[i, c, y, k, :, YC] if part == "Y" else yb_ref.at[i, c, :, k, :, ZC]

    def g_line(part, i, par, j):
        for s in "+-":
            yes, k = ag_send(s, j)

            @pl.when(yes)
            def _():
                rdma(f"g{part}{s}{j}", lax.rem(i, 4), g_src(part, i, k), g_src(part, i, k), s).start()

    def g_wait(part, i, par, j):
        for s in "+-":
            yes, k = ag_send(s, j)
            got, _ = ag_recv(s, j)
            ref = g_src(part, i, 0)
            cp = rdma(f"g{part}{s}{j}", lax.rem(i, 4), ref, ref, s)
            pl.when(yes)(cp.wait_send)
            pl.when(got)(cp.wait_recv)

    def s5(i, par):
        och_copy(i).wait()
        lines, rung = ag_first(i, par)
        for yes, got, cp in lines:
            pl.when(yes)(cp.wait_send)
            pl.when(got)(cp.wait_recv)
        g_rung(i, "0").wait_send()
        g_line("Y", i, par, 2)
        g_rungs(i, 1)
        rung.wait()
        g_line("Z", i, par, 1)

    def s6(i, par):
        g_wait("Y", i, par, 2)
        g_line("Y", i, par, 3)
        g_rungs(i, 2)
        g_wait("Z", i, par, 1)
        g_line("Z", i, par, 2)

    def g_rung(i, name, k=0):
        ref = yb_ref.at[i, c, y, k, :, YC]
        return rdma("gR" + name, lax.rem(i, 4), och.at[:, YC] if name == "0" else ref, yb_ref.at[i, c, y, z, :, YC] if name == "0" else ref, "y")

    def g_rungs(i, j):
        for s in "+-":
            got, k = ag_recv(s, j)
            pl.when(got)(lambda: g_rung(i, f"{s}{j}", k).start())

    def g_core(i, par):
        ref = yb_ref.at[i, c]
        return rdma("gD", lax.rem(i, 4), ref, ref, "c")

    def s7(i, par):
        g_wait("Y", i, par, 3)
        g_rungs(i, 3)
        g_wait("Z", i, par, 2)
        g_line("Z", i, par, 3)

    def s8(i, par):
        g_wait("Z", i, par, 3)
        g_rung(i, "0").wait_recv()
        for j in (1, 2, 3):
            for s in "+-":
                pl.when(ag_recv(s, j)[0])(lambda: g_rung(i, f"{s}{j}").wait())
        g_core(i, par).start()

    def s9(i, par):
        g_core(i, par).wait()

    actions = [("sd", sd), ("s0", s0), ("s1", s1), ("s2", s2), ("s3", s3), ("s4", s4), ("s5", s5), ("s6", s6), ("s7", s7), ("s8", s8), ("s9", s9)]
    order = sorted(actions, key=lambda a: -AT[a[0]][0])

    CR = {"c": 0, "y": 1, "-": 2, "+": 3}
    BACK = {"c": 0, "y": 1, "-": 3, "+": 2}

    rows_start(0)
    fetch(0)
    fetch(1)
    for n, ref in enumerate((ga_ref, gm_ref)):
        for q in range(D // HEAD):
            gain[n, :, q * HEAD : (q + 1) * HEAD] = jnp.broadcast_to(ref[q : q + 1, :].astype(F32), (8, HEAD))

    def turns(g, _):
        shape = (64, HEAD)
        lane = lax.broadcasted_iota(jnp.int32, shape, 1)
        place = (lax.broadcasted_iota(jnp.int32, shape, 0) + g * 64).astype(F32)
        angle = place * jnp.exp(lax.rem(lane, HEAD // 2).astype(F32) * (-math.log(THETA) / (HEAD // 2)))
        rows = pl.ds(pl.multiple_of(g * 64, 64), 64)
        cos_ref[rows, :] = jnp.cos(angle)
        sin_ref[rows, :] = jnp.where(lane < HEAD // 2, -1.0, 1.0) * jnp.sin(angle)

    lax.fori_loop(0, 2 * JR // 64, turns, None)

    def parts_by(m):
        n = jnp.maximum(m - 1, 0)

        def over(start, a, b, most):
            return jnp.minimum(lax.div(jnp.maximum(n - start, 0) * a, b), most)

        return jnp.minimum(m, 1) * NP + over(0, 9, 7, NP) + over(7, 1, 1, NP) + over(16, 9, 14, (NJ - 2) * NP) + over(AT_MLP, 16, 21, MP * NJ)

    def compute(n, _):
        ends = (NJ + 1) * NP

        @pl.when(n < ends)
        def _():
            step, part = lax.div(n, NP), lax.rem(n, NP)
            pl.when((part == 2) & (step >= 1))(lambda: rows_start(step))
            pl.when(step < 2)(lambda: attention_part(step, part, R))
            pl.when(step >= 2)(lambda: attention_part(step, part, JR))

        @pl.when(n >= ends)
        def _():
            job, part = NJ + lax.div(n - ends, MP), lax.rem(n - ends, MP)
            pl.when(part == 4)(lambda: rows_start(job + 1))
            mlp_part(job, part)

    def body(m, _):
        k, n = lax.div(m + NS - 1, NS) - 1, lax.rem(m + NS - 1, NS)
        pl.when((n == 0) & (k >= 1) & (k <= LAST_CREDIT))(lambda: each_peer(lambda p: pl.semaphore_wait(cred.at[CR[p]], 1)))
        for name, fn in order:
            d, pos = AT[name]
            i = k - d
            pl.when((n == pos) & (i >= 0) & (i < NT))(lambda fn=fn, i=i: fn(i, lax.rem(i, 2)))
        lax.fori_loop(parts_by(m), parts_by(m + 1), compute, None)
        pl.when((n == 5) & (k >= 0) & (k < LAST_CREDIT))(lambda: each_peer(lambda p: signal(cred.at[BACK[p]], p)))

    lax.fori_loop(0, LAST * NS + AT["s9"][1] + 2, body, None)


def solution(mesh):
    def step(x, gain_a, wq, wk, wv, wo, gain_m, w_gate, w_up, w_down):
        batch, rows, d = x.shape
        hbm, vmem = pl.BlockSpec(memory_space=pl.ANY), pl.BlockSpec(memory_space=pltpu.VMEM)
        yb = pl.pallas_call(
            kernel,
            out_shape=jax.ShapeDtypeStruct((NT, 2, 2, 4, C, D), BF16),
            in_specs=[hbm, hbm, vmem, vmem] + [hbm] * 7,
            out_specs=hbm,
            scratch_shapes=[
                pltpu.VMEM((OS, 2, 4, C, D), F32),
                pltpu.VMEM((OT, 2, 4, C, D), BF16),
                pltpu.VMEM((2, 2, 4, C, D), BF16),
                pltpu.VMEM((2, 4, C, CY), BF16),
                pltpu.VMEM((4, 4, C, CY), BF16),
                pltpu.VMEM((2, 3, C, CY), BF16),
                pltpu.VMEM((2, 2, 3, C, CY), BF16),
                pltpu.VMEM((2, 3, 2, C, CZ), BF16),
                pltpu.VMEM((2, 2, 3, 2, C, CZ), BF16),
                pltpu.VMEM((C, CZ), BF16),
                pltpu.VMEM((2, C, CZ), BF16),
                pltpu.VMEM((C, D), BF16),
                pltpu.VMEM((C, D), BF16),
                pltpu.VMEM((NI, C, D), BF16),
                pltpu.VMEM((2, JR, D), BF16),
                pltpu.VMEM((WS, KH, PW), BF16),
                pltpu.VMEM((2, JR, FL), F32),
                pltpu.VMEM((JR, FL), BF16),
                pltpu.VMEM((HW // HEAD, 2 * JR, HEAD), BF16),
                pltpu.VMEM((HW // HEAD, 2 * JR, HEAD), BF16),
                pltpu.VMEM((JR, HW), BF16),
                pltpu.VMEM((2, 8, D), F32),
                pltpu.VMEM((2 * JR, HEAD), F32),
                pltpu.VMEM((2 * JR, HEAD), F32),
                pltpu.SemaphoreType.DMA((len(SEMS), 4)),
                pltpu.SemaphoreType.DMA((len(SEMS), 4)),
                pltpu.SemaphoreType.REGULAR((4,)),
                pltpu.SemaphoreType.DMA((WS,)),
                pltpu.SemaphoreType.DMA((2,)),
                pltpu.SemaphoreType.DMA,
                pltpu.SemaphoreType.DMA,
            ],
            compiler_params=pltpu.CompilerParams(collective_id=0, has_side_effects=True, vmem_limit_bytes=67043328),
            name="layer",
        )(x.reshape(NI, 2, 2, 4, C, D), x.reshape(NJ, JR, D), gain_a.reshape(-1, HEAD), gain_m.reshape(-1, HEAD), wq, wk, wv, wo, w_gate, w_up, w_down)
        return yb[NI:].reshape(x.shape)

    tokens, whole, columns, rows_of = P("dp", None, None), P(None), P(None, "tp"), P("tp", None)
    return jax.shard_map(
        step,
        mesh=mesh,
        in_specs=(tokens, whole, columns, columns, columns, rows_of, whole, columns, columns, rows_of),
        out_specs=tokens,
        check_vma=False,
    )
```

```python
import functools
import math

import jax
import jax.numpy as jnp
from jax import lax
from jax.experimental import pallas as pl
from jax.experimental.pallas import tpu as pltpu
from jax.sharding import PartitionSpec as P

HEAD = 128
THETA = 10000
F32, BF16 = jnp.float32, jnp.bfloat16

JR = 256
R = JR // 2
RH = R // 2
C = RH // 8
NJ = 8
NI = 2 * NJ
NT = 2 * NI
OS = 7
OT = 4
WS = 4
MP = 13
NP = 9
AT_MLP = 100
D, HW, FL = 8192, 512, 1536
CY = 4992
CZ = D - CY
KH, GK, PW = D // 2, 1024, 512
NS = 8
AT = {"sd": (0, 0), "s0": (0, 2), "s1": (0, 6), "s2": (1, 3), "s3": (2, 0), "s4": (2, 4), "s5": (3, 1), "s6": (3, 5), "s7": (4, 2), "s8": (4, 6), "s9": (5, 0)}
LAST = NT - 1 + AT["s9"][0]
LAST_CREDIT = NT - 1 + AT["s3"][0]

SEMS = ["D", "ZR", "gZR", "gD", "gR0"] + [f"YR{q}" for q in range(4)] + [f"gR{s}{j}" for s in "+-" for j in (1, 2, 3)] + [f"{g}{p}{s}{j}" for g in ("", "g") for p in "YZ" for s in "+-" for j in (1, 2, 3)]
SEM = {n: i for i, n in enumerate(SEMS)}


def _dot(a, b, ca=1, cb=0):
    return lax.dot_general(a, b, (((ca,), (cb,)), ((), ())), preferred_element_type=F32)


def kernel(x_ref, xj_ref, ga_ref, gm_ref, wq_ref, wk_ref, wv_ref, wo_ref, wg_ref, wu_ref, wd_ref, yb_ref,
           own, oth, drx, yrs, yrr, yls, ylr, zls, zlr, zrs, zrr, och, xch, hst, ablk, wsl, acc, hid, kst, vst, seen, gain, cos_ref, sin_ref,
           ssem, rsem, cred, wsem, asem, xsem, osem):
    t = lax.axis_index("tp")
    c, z, y = lax.rem(t, 2), lax.rem(lax.div(t, 2), 4), lax.div(t, 8)

    def at(y_, z_, c_):
        return (y_ * 4 + z_) * 2 + c_

    peer = {"c": at(y, z, 1 - c), "y": at(1 - y, z, c), "+": at(y, jnp.minimum(z + 1, 3), c), "-": at(y, jnp.maximum(z - 1, 0), c)}

    def signal(sem, to):
        pl.semaphore_signal(sem, inc=1, device_id={"tp": peer[to]}, device_id_type=pl.DeviceIdType.MESH)

    def each_peer(fn):
        fn("c")
        fn("y")
        pl.when(z > 0)(lambda: fn("-"))
        pl.when(z < 3)(lambda: fn("+"))

    barrier = pltpu.get_barrier_semaphore()
    each_peer(lambda p: signal(barrier, p))
    pl.when((z == 0) | (z == 3))(lambda: pl.semaphore_wait(barrier, 3))
    pl.when((z > 0) & (z < 3))(lambda: pl.semaphore_wait(barrier, 4))

    def rdma(name, par, src, dst, to):
        return pltpu.make_async_remote_copy(src_ref=src, dst_ref=dst, send_sem=ssem.at[SEM[name], par], recv_sem=rsem.at[SEM[name], par],
                                            device_id={"tp": peer[to]}, device_id_type=pl.DeviceIdType.MESH)

    NA = (NJ + 1) * 8
    NW = NA + NJ * 24

    def fetch(w):
        slot = lax.rem(w, WS)
        sem = wsem.at[slot]

        def go(src, lo, n):
            pltpu.make_async_copy(src, wsl.at[slot, pl.ds(lo, n), :], sem).start()

        @pl.when(w < NA)
        def _():
            j = lax.rem(w, 8)
            h = lax.rem(j, 2)
            for n, ref in enumerate((wq_ref, wk_ref, wv_ref)):
                pl.when(lax.div(j, 2) == n)(lambda ref=ref: go(ref.at[pl.ds(h * KH, KH), :], 0, KH))

            @pl.when(j >= 6)
            def _():
                for p in range(8):
                    go(wo_ref.at[:, pl.ds(h * KH + p * PW, PW)], p * HW, HW)

        @pl.when((w >= NA) & (w < NW))
        def _():
            u = lax.rem(w - NA, 24)
            for n, ref in enumerate((wg_ref, wu_ref)):
                @pl.when((u < 16) & (lax.rem(u, 2) == n))
                def _(ref=ref):
                    for p in range(3):
                        go(ref.at[pl.ds(lax.div(u, 2) * GK, GK), pl.ds(p * PW, PW)], p * GK, GK)

            @pl.when(u >= 16)
            def _():
                for p in range(2):
                    go(wd_ref.at[:, pl.ds((u - 16) * 2 * PW + p * PW, PW)], p * FL, FL)

    def tile_wait(w, rows):
        slot = lax.rem(w, WS)
        ref = wsl.at[slot, pl.ds(0, rows), :]
        pltpu.make_async_copy(ref, ref, wsem.at[slot]).wait()
        return slot

    def rows_start(job):
        slot = lax.rem(job, 2)

        def eight(q, _):
            item, u, v = lax.div(q, 16), lax.rem(lax.div(q, 4), 2), lax.rem(q, 4)

            half = lax.rem(lax.div(q, 8), 2)
            src = yb_ref.at[2 * (job - NJ) + item, lax.rem(c + half, 2), u, v]
            at_row = pl.multiple_of(half * R + item * RH + (u * 4 + v) * C, C)
            pltpu.make_async_copy(src, ablk.at[slot, pl.ds(at_row, C), :], asem.at[slot]).start()

        pl.when(job < NJ)(pltpu.make_async_copy(xj_ref.at[jnp.minimum(job, NJ - 1)], ablk.at[slot], asem.at[slot]).start)
        pl.when((job >= NJ) & (job < 2 * NJ))(lambda: lax.fori_loop(0, 32, eight, None))

    def rows_wait(job):
        slot = lax.rem(job, 2)
        pltpu.make_async_copy(ablk.at[slot], ablk.at[slot], asem.at[slot]).wait()

    def first_rows(h):
        rows = pl.ds(h * R, R)
        return pltpu.make_async_copy(xj_ref.at[0, rows, :], ablk.at[0, rows, :], asem.at[2 * h])

    def put(item, out, col):
        cols = pl.ds(pl.multiple_of(col, PW), PW)
        n = out.shape[0] // R
        for q in range(n):
            own[lax.rem(item + q, OS), :, :, :, cols] = out[q * RH : (q + 1) * RH].reshape(2, 4, C, PW)
            oth[lax.rem(item + q, OT), :, :, :, cols] = out[(n + q) * RH : (n + q + 1) * RH].reshape(2, 4, C, PW).astype(BF16)

    def attention_part(step, n, size):
        job = jnp.maximum(step - 1, 0)
        item = step if size == R else 2 * job
        at_row = step * R if size == R else 0
        mine = pl.ds(pl.multiple_of(at_row, R), size)
        ab = lax.rem(job, 2)
        half = lax.rem(job, 2)
        w = step * 8

        if size == R:
            @pl.when((n == 0) & (step == 0))
            def _():
                first_rows(0).wait()
                for q in range(2, WS):
                    fetch(q)

            pl.when((n == 5) & (step == 0))(first_rows(1).start)
            pl.when((n == 0) & (step == 1))(first_rows(1).wait)
        else:
            pl.when(n == 0)(lambda: rows_wait(job))

        @pl.when(n < size // R)
        def _():
            def norm(g, _):
                rows = pl.ds(pl.multiple_of(at_row + n * R + g * 32, 32), 32)
                total = jnp.zeros((32, HEAD), F32)
                for j in range(0, D, GK):
                    v = ablk[ab, rows, j : j + GK].astype(F32)
                    v = v * v
                    for q in range(0, GK, HEAD):
                        total += v[:, q : q + HEAD]
                scale = lax.rsqrt(jnp.sum(total, -1, keepdims=True) * (1 / D) + 1e-6)
                for j in range(0, D, GK):
                    v = ablk[ab, rows, j : j + GK].astype(F32) * scale
                    v = v.reshape(4, 8, GK) * gain[0, :, j : j + GK]
                    ablk[ab, rows, j : j + GK] = v.reshape(32, GK).astype(BF16)

            lax.fori_loop(0, R // 32, norm, None)

        @pl.when((n >= 2) & (n < 5))
        def _():
            tile = w + (n - 2) * 2
            slots = [tile_wait(tile + q, KH) for q in range(2)]
            cols = pl.ds(pl.multiple_of((n - 2) * PW, PW), PW)
            acc[0, mine, cols] = _dot(ablk[ab, mine, :KH], wsl[slots[0]]) + _dot(ablk[ab, mine, KH:], wsl[slots[1]])
            for q in range(2):
                fetch(tile + q + WS)

        @pl.when((n == 5) | (n == 6))
        def _():
            first = (n - 5) * 2
            col = pl.multiple_of(first * HEAD, 2 * HEAD)
            place = pl.ds(pl.multiple_of(half * JR + at_row, R), size)
            cos, sin = cos_ref[place, :], sin_ref[place, :]

            def column(at_col, i):
                return acc[0, mine, pl.ds(pl.multiple_of(at_col + col + i * HEAD, HEAD), HEAD)].astype(BF16)

            def turn(at_col, i):
                v = column(at_col, i).astype(F32)
                return (v * cos + pltpu.roll(v, HEAD // 2, 1) * sin).astype(BF16)

            qs = [turn(0, i) for i in range(2)]
            for i in range(2):
                kst[first + i, place, :] = turn(PW, i)
                vst[first + i, place, :] = column(2 * PW, i)

            def attend(seen_keys):
                for i in range(2):
                    s = _dot(qs[i], kst[first + i, :seen_keys, :], 1, 1) * HEAD**-0.5
                    token = lax.broadcasted_iota(jnp.int32, s.shape, 0) + (seen_keys - size)
                    s = jnp.where(token >= lax.broadcasted_iota(jnp.int32, s.shape, 1), s, -jnp.inf)
                    p = jnp.exp(s - s.max(-1, keepdims=True))
                    p = (p * (1 / p.sum(-1, keepdims=True))).astype(BF16)
                    o = _dot(p, vst[first + i, :seen_keys, :]).astype(BF16)
                    for h in range(size // RH):
                        to_row = lax.rem(c + h, 2) * (size // 2) + (h // 2) * RH
                        seen[pl.ds(pl.multiple_of(to_row, RH), RH), pl.ds(pl.multiple_of(col + i * HEAD, HEAD), HEAD)] = o[h * RH : (h + 1) * RH]

            early = step == 0 if size == R else half == 0
            pl.when(early)(lambda: attend(size))
            pl.when(~early)(lambda: attend(2 * size))

        @pl.when(n >= 7)
        def _():
            tile = w + n - 1
            slot = tile_wait(tile, KH)
            for p in range(8):
                put(item, _dot(seen[:size], wsl[slot, p * HW : (p + 1) * HW, :]), (n - 7) * KH + p * PW)
            fetch(tile + WS)

    def mlp_part(job, u):
        ab = lax.rem(job, 2)
        w = NA + (job - NJ) * 24 + 2 * jnp.where(u < 8, u, u - 1)

        @pl.when(u == 0)
        def _():
            rows_wait(job)
            acc[...] = jnp.zeros((2, JR, FL), F32)

        @pl.when(u < 8)
        def _():
            slots = [tile_wait(w + q, 3 * GK) for q in range(2)]
            lhs = ablk[ab, :, pl.ds(pl.multiple_of(u * GK, GK), GK)]
            for q in range(2):
                for p in range(3):
                    acc[q, :, p * PW : (p + 1) * PW] += _dot(lhs, wsl[slots[q], p * GK : (p + 1) * GK, :])
            for q in range(2):
                fetch(w + q + WS)

        @pl.when(u == 8)
        def _():
            def rows(g, _):
                r = pl.ds(pl.multiple_of(g * 16, 16), 16)
                gate = acc[0, r, :]
                hid[r, :] = (gate * (1 / (1 + jnp.exp(-gate))) * acc[1, r, :]).astype(BF16)

            lax.fori_loop(0, JR // 16, rows, None)

        @pl.when(u > 8)
        def _():
            slots = [tile_wait(w + q, 3 * GK) for q in range(2)]
            for q in range(2):
                for p in range(2):
                    put(2 * job, _dot(hid[...], wsl[slots[q], p * FL : (p + 1) * FL, :]), ((u - 9) * 2 + q) * 2 * PW + p * PW)
            for q in range(2):
                fetch(w + q + WS)

    def rs_send(s, j):
        return ((z < 3) & (j > z), 4 + z - j) if s == "+" else ((z > 0) & (j >= 4 - z), j + z - 4)

    def rs_recv(s, j):
        return (z >= 1) & (j >= z) if s == "+" else (z <= 2) & (j >= 3 - z)

    def first(s):
        return z == 0 if s == "+" else z == 3

    def ag_send(s, j):
        return ((z < 3) & (j <= z + 1), z - (j - 1)) if s == "+" else ((z > 0) & (j <= 4 - z), z + (j - 1))

    def ag_recv(s, j):
        return ((z >= 1) & (j <= z), z - j) if s == "+" else ((z <= 2) & (j <= 3 - z), z + j)

    YC, ZC = pl.ds(0, CY), pl.ds(CY, CZ)
    S = {"+": 0, "-": 1}

    def core(i, par):
        return rdma("D", par, oth.at[lax.rem(i, OT)], drx.at[par], "c")

    def sd(i, par):
        pl.when((i < 2) | (par == 0))(core(i, par).start)
        pl.when((i >= 2) & (par == 0))(core(i + 1, 1).start)

    def y_line(i, par, j):
        for s in "+-":
            yes, k = rs_send(s, j)

            @pl.when(yes & first(s))
            def _():
                yls[S[s], j - 1] = own[lax.rem(i, OS), y, k, :, YC].astype(BF16)

            if j > 1:
                @pl.when(yes & ~first(s))
                def _():
                    yls[S[s], j - 1] = (own[lax.rem(i, OS), y, k, :, YC] + ylr[par, S[s], j - 2].astype(F32)).astype(BF16)

            pl.when(yes)(rdma(f"Y{s}{j}", par, yls.at[S[s], j - 1], ylr.at[par, S[s], j - 1], s).start)

    def z_line(i, par, j):
        for s in "+-":
            yes, k = rs_send(s, j)

            @pl.when(yes & first(s))
            def _():
                for h in range(2):
                    zls[S[s], j - 1, h] = own[lax.rem(i, OS), h, k, :, ZC].astype(BF16)

            if j > 1:
                @pl.when(yes & ~first(s))
                def _():
                    for h in range(2):
                        zls[S[s], j - 1, h] = (own[lax.rem(i, OS), h, k, :, ZC] + zlr[par, S[s], j - 2, h].astype(F32)).astype(BF16)

            pl.when(yes)(rdma(f"Z{s}{j}", par, zls.at[S[s], j - 1], zlr.at[par, S[s], j - 1], s).start)

    def line_wait(part, par, j):
        sb, rb = (yls, ylr) if part == "Y" else (zls, zlr)
        for s in "+-":
            cp = rdma(f"{part}{s}{j}", par, sb.at[S[s], j - 1], rb.at[par, S[s], j - 1], s)
            pl.when(rs_send(s, j)[0])(cp.wait_send)
            pl.when(rs_recv(s, j))(cp.wait_recv)

    def piece(q):
        return (jnp.where(z < 2, 3, 0), jnp.where(z < 2, 2, 1), jnp.where(z < 2, 1 - z, 5 - z), z)[q]

    def rung(i, par, q):
        four = lax.rem(i, 4)
        return rdma(f"YR{q}", four, yrs.at[par, q], yrr.at[four, q], "y")

    def rung_add(i, par, q):
        rung(i, par, q).wait_recv()
        own[lax.rem(i, OS), y, piece(q), :, YC] += yrr[lax.rem(i, 4), q].astype(F32)

    def s0(i, par):
        core(i, par).wait()
        slot = lax.rem(i, OS)

        def add(k, _):
            a, b = lax.div(k, 4), lax.rem(k, 4)
            own[slot, a, b] += drx[par, a, b].astype(F32)

        lax.fori_loop(0, 8, add, None)

        for q in range(4):
            yrs[par, q] = own[slot, 1 - y, piece(q), :, YC].astype(BF16)
            rung(i, par, q).start()
            if q == 0:
                z_line(i, par, 1)

    def s1(i, par):
        rung_add(i, par, 0)
        y_line(i, par, 1)
        line_wait("Z", par, 1)
        z_line(i, par, 2)

    def s2(i, par):
        for q in range(4):
            rung(i, par, q).wait_send()
        rung_add(i, par, 1)
        line_wait("Y", par, 1)
        y_line(i, par, 2)
        line_wait("Z", par, 2)
        z_line(i, par, 3)

    def x_copy(i):
        return pltpu.make_async_copy(x_ref.at[i, c, y, z], xch, xsem)

    def s3(i, par):
        pl.when(i < NI)(lambda: x_copy(i).start())
        rung_add(i, par, 2)
        line_wait("Y", par, 2)
        y_line(i, par, 3)
        line_wait("Z", par, 3)
        slot = lax.rem(i, OS)
        for s in "+-":
            @pl.when(rs_recv(s, 3))
            def _():
                for h in range(2):
                    own[slot, h, z, :, ZC] += zlr[par, S[s], 2, h].astype(F32)
        zrs[...] = own[slot, 1 - y, z, :, ZC].astype(BF16)
        rdma("ZR", par, zrs, zrr.at[par], "y").start()

    def och_copy(i):
        return pltpu.make_async_copy(och, yb_ref.at[i, c, y, z], osem)

    def ag_first(i, par):
        cps = [(ag_send(s, 1)[0], ag_recv(s, 1)[0], rdma(f"gY{s}1", lax.rem(i, 4), och.at[:, YC], yb_ref.at[i, c, y, z, :, YC], s)) for s in "+-"]
        return cps, rdma("gZR", lax.rem(i, 4), och.at[:, ZC], yb_ref.at[i, c, y, z, :, ZC], "y")

    def s4(i, par):
        slot = lax.rem(i, OS)
        rung_add(i, par, 3)
        line_wait("Y", par, 3)
        for s in "+-":
            @pl.when(rs_recv(s, 3))
            def _():
                own[slot, y, z, :, YC] += ylr[par, S[s], 2].astype(F32)
        rdma("ZR", par, zrs, zrr.at[par], "y").wait()
        own[slot, y, z, :, ZC] += zrr[par].astype(F32)

        @pl.when(i < NI)
        def _():
            x_copy(i).wait()
            h = (xch[...].astype(F32) + own[slot, y, z]).astype(BF16)
            hst[i] = h
            v = h.astype(F32)
            scale = lax.rsqrt(jnp.mean(v * v, -1, keepdims=True) + 1e-6)
            och[...] = (v * scale * gain[1]).astype(BF16)

        @pl.when(i >= NI)
        def _():
            och[...] = (hst[i - NI].astype(F32) + own[slot, y, z]).astype(BF16)

        och_copy(i).start()
        lines, rung = ag_first(i, par)
        for yes, _, cp in lines:
            pl.when(yes)(cp.start)
        g_rung(i, "0").start()
        rung.start()

    def ag_y(i, par, j):
        return [(*ag_send(s, j), *ag_recv(s, j), s) for s in "+-"]

    def g_src(part, i, k):
        return yb_ref.at[i, c, y, k, :, YC] if part == "Y" else yb_ref.at[i, c, :, k, :, ZC]

    def g_line(part, i, par, j):
        for s in "+-":
            yes, k = ag_send(s, j)

            @pl.when(yes)
            def _():
                rdma(f"g{part}{s}{j}", lax.rem(i, 4), g_src(part, i, k), g_src(part, i, k), s).start()

    def g_wait(part, i, par, j):
        for s in "+-":
            yes, k = ag_send(s, j)
            got, _ = ag_recv(s, j)
            ref = g_src(part, i, 0)
            cp = rdma(f"g{part}{s}{j}", lax.rem(i, 4), ref, ref, s)
            pl.when(yes)(cp.wait_send)
            pl.when(got)(cp.wait_recv)

    def s5(i, par):
        och_copy(i).wait()
        lines, rung = ag_first(i, par)
        for yes, got, cp in lines:
            pl.when(yes)(cp.wait_send)
            pl.when(got)(cp.wait_recv)
        g_rung(i, "0").wait_send()
        g_line("Y", i, par, 2)
        g_rungs(i, 1)
        rung.wait()
        g_line("Z", i, par, 1)

    def s6(i, par):
        g_wait("Y", i, par, 2)
        g_line("Y", i, par, 3)
        g_rungs(i, 2)
        g_wait("Z", i, par, 1)
        g_line("Z", i, par, 2)

    def g_rung(i, name, k=0):
        ref = yb_ref.at[i, c, y, k, :, YC]
        return rdma("gR" + name, lax.rem(i, 4), och.at[:, YC] if name == "0" else ref, yb_ref.at[i, c, y, z, :, YC] if name == "0" else ref, "y")

    def g_rungs(i, j):
        for s in "+-":
            got, k = ag_recv(s, j)
            pl.when(got)(lambda: g_rung(i, f"{s}{j}", k).start())

    def g_core(i, par):
        ref = yb_ref.at[i, c]
        return rdma("gD", lax.rem(i, 4), ref, ref, "c")

    def s7(i, par):
        g_wait("Y", i, par, 3)
        g_rungs(i, 3)
        g_wait("Z", i, par, 2)
        g_line("Z", i, par, 3)

    def s8(i, par):
        g_wait("Z", i, par, 3)
        g_rung(i, "0").wait_recv()
        for j in (1, 2, 3):
            for s in "+-":
                pl.when(ag_recv(s, j)[0])(lambda: g_rung(i, f"{s}{j}").wait())
        g_core(i, par).start()

    def s9(i, par):
        g_core(i, par).wait()

    actions = [("sd", sd), ("s0", s0), ("s1", s1), ("s2", s2), ("s3", s3), ("s4", s4), ("s5", s5), ("s6", s6), ("s7", s7), ("s8", s8), ("s9", s9)]
    order = sorted(actions, key=lambda a: -AT[a[0]][0])

    CR = {"c": 0, "y": 1, "-": 2, "+": 3}
    BACK = {"c": 0, "y": 1, "-": 3, "+": 2}

    first_rows(0).start()
    fetch(0)
    fetch(1)
    for n, ref in enumerate((ga_ref, gm_ref)):
        for q in range(D // HEAD):
            gain[n, :, q * HEAD : (q + 1) * HEAD] = jnp.broadcast_to(ref[q : q + 1, :].astype(F32), (8, HEAD))

    def turns(g, _):
        shape = (64, HEAD)
        lane = lax.broadcasted_iota(jnp.int32, shape, 1)
        place = (lax.broadcasted_iota(jnp.int32, shape, 0) + g * 64).astype(F32)
        angle = place * jnp.exp(lax.rem(lane, HEAD // 2).astype(F32) * (-math.log(THETA) / (HEAD // 2)))
        rows = pl.ds(pl.multiple_of(g * 64, 64), 64)
        cos_ref[rows, :] = jnp.cos(angle)
        sin_ref[rows, :] = jnp.where(lane < HEAD // 2, -1.0, 1.0) * jnp.sin(angle)

    lax.fori_loop(0, 2 * JR // 64, turns, None)

    def parts_by(m):
        n = jnp.maximum(m - 1, 0)

        def over(start, a, b, most):
            return jnp.minimum(lax.div(jnp.maximum(n - start, 0) * a, b), most)

        return jnp.minimum(m, 1) * NP + over(0, 9, 7, NP) + over(7, 1, 1, NP) + over(16, 9, 14, (NJ - 2) * NP) + over(AT_MLP, 16, 21, MP * NJ)

    def compute(n, _):
        ends = (NJ + 1) * NP

        @pl.when(n < ends)
        def _():
            step, part = lax.div(n, NP), lax.rem(n, NP)
            pl.when((part == 2) & (step >= 1))(lambda: rows_start(step))
            pl.when(step < 2)(lambda: attention_part(step, part, R))
            pl.when(step >= 2)(lambda: attention_part(step, part, JR))

        @pl.when(n >= ends)
        def _():
            job, part = NJ + lax.div(n - ends, MP), lax.rem(n - ends, MP)
            pl.when(part == 4)(lambda: rows_start(job + 1))
            mlp_part(job, part)

    def body(m, _):
        k, n = lax.div(m + NS - 1, NS) - 1, lax.rem(m + NS - 1, NS)
        pl.when((n == 0) & (k >= 1) & (k <= LAST_CREDIT))(lambda: each_peer(lambda p: pl.semaphore_wait(cred.at[CR[p]], 1)))
        for name, fn in order:
            d, pos = AT[name]
            i = k - d
            pl.when((n == pos) & (i >= 0) & (i < NT))(lambda fn=fn, i=i: fn(i, lax.rem(i, 2)))
        lax.fori_loop(parts_by(m), parts_by(m + 1), compute, None)
        pl.when((n == 5) & (k >= 0) & (k < LAST_CREDIT))(lambda: each_peer(lambda p: signal(cred.at[BACK[p]], p)))

    lax.fori_loop(0, LAST * NS + AT["s9"][1] + 2, body, None)


def solution(mesh):
    def step(x, gain_a, wq, wk, wv, wo, gain_m, w_gate, w_up, w_down):
        batch, rows, d = x.shape
        hbm, vmem = pl.BlockSpec(memory_space=pl.ANY), pl.BlockSpec(memory_space=pltpu.VMEM)
        yb = pl.pallas_call(
            kernel,
            out_shape=jax.ShapeDtypeStruct((NT, 2, 2, 4, C, D), BF16),
            in_specs=[hbm, hbm, vmem, vmem] + [hbm] * 7,
            out_specs=hbm,
            scratch_shapes=[
                pltpu.VMEM((OS, 2, 4, C, D), F32),
                pltpu.VMEM((OT, 2, 4, C, D), BF16),
                pltpu.VMEM((2, 2, 4, C, D), BF16),
                pltpu.VMEM((2, 4, C, CY), BF16),
                pltpu.VMEM((4, 4, C, CY), BF16),
                pltpu.VMEM((2, 3, C, CY), BF16),
                pltpu.VMEM((2, 2, 3, C, CY), BF16),
                pltpu.VMEM((2, 3, 2, C, CZ), BF16),
                pltpu.VMEM((2, 2, 3, 2, C, CZ), BF16),
                pltpu.VMEM((C, CZ), BF16),
                pltpu.VMEM((2, C, CZ), BF16),
                pltpu.VMEM((C, D), BF16),
                pltpu.VMEM((C, D), BF16),
                pltpu.VMEM((NI, C, D), BF16),
                pltpu.VMEM((2, JR, D), BF16),
                pltpu.VMEM((WS, KH, PW), BF16),
                pltpu.VMEM((2, JR, FL), F32),
                pltpu.VMEM((JR, FL), BF16),
                pltpu.VMEM((HW // HEAD, 2 * JR, HEAD), BF16),
                pltpu.VMEM((HW // HEAD, 2 * JR, HEAD), BF16),
                pltpu.VMEM((JR, HW), BF16),
                pltpu.VMEM((2, 8, D), F32),
                pltpu.VMEM((2 * JR, HEAD), F32),
                pltpu.VMEM((2 * JR, HEAD), F32),
                pltpu.SemaphoreType.DMA((len(SEMS), 4)),
                pltpu.SemaphoreType.DMA((len(SEMS), 4)),
                pltpu.SemaphoreType.REGULAR((4,)),
                pltpu.SemaphoreType.DMA((WS,)),
                pltpu.SemaphoreType.DMA((3,)),
                pltpu.SemaphoreType.DMA,
                pltpu.SemaphoreType.DMA,
            ],
            compiler_params=pltpu.CompilerParams(collective_id=0, has_side_effects=True, vmem_limit_bytes=67043328),
            name="layer",
        )(x.reshape(NI, 2, 2, 4, C, D), x.reshape(NJ, JR, D), gain_a.reshape(-1, HEAD), gain_m.reshape(-1, HEAD), wq, wk, wv, wo, w_gate, w_up, w_down)
        return yb[NI:].reshape(x.shape)

    tokens, whole, columns, rows_of = P("dp", None, None), P(None), P(None, "tp"), P("tp", None)
    return jax.shard_map(
        step,
        mesh=mesh,
        in_specs=(tokens, whole, columns, columns, columns, rows_of, whole, columns, columns, rows_of),
        out_specs=tokens,
        check_vma=False,
    )
```
